128 devices in a mesh: facet: 16 (over y, x_lo, core), col: 8 (over x_hi, z).
Axes of the slice: x: 4 (x_hi: 2, x_lo: 2; x = x_hi * 2 + x_lo), y: 4, z: 4, core: 2. Of those that a mesh axis runs over, the one named last changes fastest.
Arguments:
- sky_image: float32 [2, 2048, 8192], P(None, ('facet', 'col')), may hold values from -6 to 6
- observed: float32 [2, 4096, 2048], P(None, 'facet', 'col'), may hold values from -4 to 4
- weights: int32 [4096, 2048], P('facet', 'col'), may hold values from 0 to 3
- facet_offsets: int32 [16, 2], replicated, may hold values from 0 to 7, as said below
- subgrid_rows: int32 [16], replicated, may hold values from 0 to 65535
- subgrid_columns: int32 [8], replicated, may hold values from 0 to 65535
Outputs:
- new_image: float32 [2, 2048, 8192], P(None, ('facet', 'col'))
- predicted: float32 [2, 4096, 2048], P(None, 'facet', 'col')
The draws below stay inside these ranges and needn't reach their ends.
Inputs may be any that keep to these rules, and one draw needn't show every extreme that they name: `facet_offsets`: each row is the (row, column) slot of one facet on a 8 x 8 layout; no two facets share a slot.
All inputs are finite; a program needn't handle non-finite values.
Results may differ from the reference program's by a relative error of at most 0.0003.
Values sent between devices are 32-bit elements; how exact they have to be, the bound alone decides.
A program may use at most 128 MiB of HBM per device.

```python
import math
import jax
import jax.numpy as jnp
from jax import lax

FN = 8192
M = 32
SLOTS = 8
FACETS = 16
FROWS = 128
NIMG = 65536
G = 256
ROW_STEP = 512
N_FACET = 16
N_COL = 8


def draw_facet_offsets(key, part):
    inner = jax.random.permutation(key, SLOTS * SLOTS - 2).astype(jnp.int32) + 1
    corners = jnp.array([0, SLOTS * SLOTS - 1], dtype=jnp.int32)
    picked = jnp.concatenate([corners, inner[:FACETS - 2]])
    order = jax.random.permutation(jax.random.fold_in(key, 11), FACETS)
    cells = picked[order]
    return jnp.stack([cells // SLOTS, cells % SLOTS], axis=1).astype(jnp.int32)


def plant(values, own_key, low, high):
    shape = values.shape
    index_at = [jax.random.randint(jax.random.fold_in(own_key, axis), (), 0, shape[axis]) for axis in range(len(shape))]
    values = values.at[tuple(index_at)].set(low)
    longest = shape.index(max(shape))
    index_at[longest] = (index_at[longest] + 1) % shape[longest]
    return values.at[tuple(index_at)].set(high)


def shard_levels(rng, shape, cuts, low, top_value):
    gain = 1.0
    for dim, shards_of in cuts:
        heights = jax.random.uniform(jax.random.fold_in(jax.random.fold_in(rng, 6), dim), (shards_of,), jnp.float32, low / len(cuts), top_value / len(cuts))
        gain = gain * jnp.repeat(jnp.exp(heights), shape[dim] // shards_of).reshape((-1,) + (1,) * (len(shape) - 1 - dim))
    return gain


def scatter_about(own_key, shape, scale, limit, split=(), kind=jnp.bfloat16):
    factor_of = shard_levels(own_key, shape, split, -0.22, 0.18) if split else 1.0
    drawn = jax.random.normal(own_key, shape, jnp.float32) * scale * factor_of
    return jnp.minimum(jnp.maximum(drawn, -limit), limit).astype(kind)


def setup_inputs(seed: int = 0) -> dict:
    seeds = jax.random.split(jax.random.key(seed), 7)
    sky_image = scatter_about(seeds[0], (2, FACETS * FROWS, FN), 1.0, 6.0, ((1, 128),), jnp.float32)
    observed = scatter_about(seeds[1], (2, N_FACET * G, N_COL * G), 0.5, 4.0, ((1, 16), (2, 8)), jnp.float32)
    weights = plant(jax.random.randint(seeds[2], (N_FACET * G, N_COL * G), 0, 4), jax.random.fold_in(seeds[2], 1), 0, 3).astype(jnp.int32)
    facet_offsets = draw_facet_offsets(jax.random.fold_in(seeds[6], 71), 0)
    subgrid_rows = plant(jax.random.randint(seeds[4], (N_FACET,), 0, NIMG), jax.random.fold_in(seeds[4], 1), 0, NIMG - 1).astype(jnp.int32)
    subgrid_columns = plant(jax.random.randint(seeds[5], (N_COL,), 0, NIMG), jax.random.fold_in(seeds[5], 1), 0, NIMG - 1).astype(jnp.int32)
    return dict(sky_image=sky_image, observed=observed, weights=weights, facet_offsets=facet_offsets, subgrid_rows=subgrid_rows, subgrid_columns=subgrid_columns)


HIGHEST = lax.Precision.HIGHEST
shrink_level = 0.5

def product(form, first, second):
    real_part = jnp.einsum(form, first[0], second[0], precision=HIGHEST) - jnp.einsum(form, first[1], second[1], precision=HIGHEST)
    imag_part = jnp.einsum(form, first[0], second[1], precision=HIGHEST) + jnp.einsum(form, first[1], second[0], precision=HIGHEST)
    return (real_part, imag_part)

def conjugate(pair):
    return (pair[0], -pair[1])

def phases(first_ids, second_ids, period, extent):
    wrapped = jnp.remainder(first_ids[:, None] * second_ids[None, :], period)
    angles = wrapped.astype(jnp.float32) * (2.0 * math.pi / period)
    factor = 1.0 / math.sqrt(extent)
    return (jnp.cos(angles) * factor, -jnp.sin(angles) * factor)

def shrink(values):
    magnitude = jnp.sqrt(values[0] * values[0] + values[1] * values[1])
    ratio = jnp.maximum(magnitude - shrink_level, 0.0) / jnp.maximum(magnitude, shrink_level)
    return values * ratio[None]

def subgrid_tables(facet_offsets, contrib, grid):
    contrib_ids = jnp.arange(contrib, dtype=jnp.int32)
    grid_ids = jnp.arange(grid, dtype=jnp.int32)
    row_place = (facet_offsets[:, 0:1] * contrib + contrib_ids[None, :]).reshape(-1)
    column_place = (facet_offsets[:, 1:2] * contrib + contrib_ids[None, :]).reshape(-1)
    downward = phases(row_place, grid_ids, grid, grid)
    sideways = phases(column_place, grid_ids, grid, grid)
    sideways = (sideways[0].reshape(-1, contrib, grid), sideways[1].reshape(-1, contrib, grid))
    return (downward, sideways)

def subgrid_predict(parts, tables):
    downward, sideways = tables
    halfway = product('fpq,fqv->fpv', (parts[:, 0], parts[:, 1]), sideways)
    flat = (halfway[0].reshape(-1, halfway[0].shape[2]), halfway[1].reshape(-1, halfway[1].shape[2]))
    return product('ku,kv->uv', downward, flat)

def subgrid_adjoint(resid, tables):
    downward, sideways = tables
    upper = product('ku,uv->kv', conjugate(downward), resid)
    facet_count = sideways[0].shape[0]
    upper = (upper[0].reshape(facet_count, -1, upper[0].shape[1]), upper[1].reshape(facet_count, -1, upper[1].shape[1]))
    back = product('fpv,fqv->fpq', upper, conjugate(sideways))
    return jnp.stack(back, axis=1)

def facet_tables(slot, subgrid_rows, subgrid_columns):
    contrib_ids = jnp.arange(M, dtype=jnp.int32)
    row_index = slot[0] * FN + jnp.arange(FROWS, dtype=jnp.int32)
    column_index = slot[1] * FN + jnp.arange(FN, dtype=jnp.int32)
    row_freq = (subgrid_rows[:, None] + ROW_STEP * contrib_ids[None, :]).reshape(-1)
    column_freq = (subgrid_columns[:, None] + SLOTS * contrib_ids[None, :]).reshape(-1)
    across = phases(row_index, row_freq, NIMG, FROWS)
    along = phases(column_index, column_freq, NIMG, FN)
    return (across, along)

def forward_facet(facet_slab, slot, subgrid_rows, subgrid_columns):
    across, along = facet_tables(slot, subgrid_rows, subgrid_columns)
    inner = product('rx,xj->rj', (facet_slab[0], facet_slab[1]), along)
    terms = product('ri,rj->ij', across, inner)
    stacked = jnp.stack(terms).reshape(2, N_FACET, M, N_COL, M)
    return stacked.transpose(1, 3, 0, 2, 4)

def reference(sky_image, observed, weights, facet_offsets, subgrid_rows, subgrid_columns):
    slabs = sky_image.reshape(2, FACETS, FROWS, FN).transpose(1, 0, 2, 3)
    tables = subgrid_tables(facet_offsets, M, G)

    def forward_all(all_slabs):

        def one_facet(packed):
            return forward_facet(packed[0], packed[1], subgrid_rows, subgrid_columns)
        terms = lax.map(one_facet, (all_slabs, facet_offsets))
        return terms.transpose(1, 2, 0, 3, 4, 5).reshape(N_FACET * N_COL, FACETS, 2, M, M)
    per_subgrid = forward_all(slabs)
    seen = observed.reshape(2, N_FACET, G, N_COL, G).transpose(1, 3, 0, 2, 4).reshape(N_FACET * N_COL, 2, G, G)
    masks = weights.reshape(N_FACET, G, N_COL, G).transpose(0, 2, 1, 3).reshape(N_FACET * N_COL, G, G).astype(jnp.float32)

    def residual_back(packed):
        parts, seen_one, mask_one = packed
        model = subgrid_predict(parts, tables)
        resid = (mask_one * (seen_one[0] - model[0]), mask_one * (seen_one[1] - model[1]))
        return subgrid_adjoint(resid, tables)
    back = lax.map(residual_back, (per_subgrid, seen, masks))
    back = back.reshape(N_FACET, N_COL, FACETS, 2, M, M).transpose(2, 3, 0, 4, 1, 5).reshape(FACETS, 2, N_FACET * M, N_COL * M)

    def update(packed):
        facet_slab, slot, back_one = packed
        across, along = facet_tables(slot, subgrid_rows, subgrid_columns)
        partial_sum = product('ri,ij->rj', conjugate(across), (back_one[0], back_one[1]))
        grads = product('rj,xj->rx', partial_sum, conjugate(along))
        return shrink(facet_slab + jnp.stack(grads))
    new_slabs = lax.map(update, (slabs, facet_offsets, back))
    new_image = new_slabs.transpose(1, 0, 2, 3).reshape(2, FACETS * FROWS, FN)
    second = forward_all(new_slabs)

    def predict_one(parts):
        return jnp.stack(subgrid_predict(parts, tables))
    predicted = lax.map(predict_one, second)
    predicted = predicted.reshape(N_FACET, N_COL, 2, G, G).transpose(2, 0, 3, 1, 4).reshape(2, N_FACET * G, N_COL * G)
    return (new_image, predicted)
```

```python
import math

import jax
import jax.numpy as jnp
from jax import lax
from jax.experimental import pallas as pl
from jax.experimental.pallas import tpu as pltpu
from jax.sharding import PartitionSpec as P

FN = 8192
M = 32
SLOTS = 8
NIMG = 65536
G = 256
FROWS = 128
NF = 16
NC = 8
SLAB = 16
LJ = 256
NI = 32
SHRINK = 0.5
F32 = jnp.float32
MESH = pl.DeviceIdType.MESH


def iota(shape, dim):
    return lax.broadcasted_iota(jnp.int32, shape, dim)


def turns(k, bits, scale):
    n = 1 << bits
    k = k & (n - 1)
    q = (k + n // 8) >> (bits - 2)
    x = (k - (q << (bits - 2))).astype(F32) * (2.0 * math.pi / n)
    y = x * x
    s = x * (1.0 + y * (-1.0 / 6 + y * (1.0 / 120 + y * (-1.0 / 5040 + y * (1.0 / 362880)))))
    c = 1.0 + y * (-0.5 + y * (1.0 / 24 + y * (-1.0 / 720 + y * (1.0 / 40320 + y * (-1.0 / 3628800)))))
    swap = (q & 1) == 1
    cc = jnp.where(swap, s, c) * scale
    ss = jnp.where(swap, c, s) * scale
    return (
        jnp.where(((q + 1) & 2) != 0, -cc, cc),
        jnp.where((q & 2) != 0, -ss, ss),
    )


def dot(a, b):
    return lax.dot_general(
        a, b, (((1,), (0,)), ((), ())),
        precision=lax.Precision.HIGH, preferred_element_type=F32,
    )


def kernel(
    offs, rows, cols, sky_h, obs_h, wts_h,
    new_h, pred_h,
    sky, obs, wts, new, pred,
    bm, bt, at, vt, vb, wz, wt, tf, pt, pk, zs, tt, rr, uu,
    send1, recv1, send2, recv2, send3, recv3, send4, recv4, send5, recv5, send6, recv6,
    ssem, rsem, isem, osem,
):
    f = lax.axis_index("facet")
    c = lax.axis_index("col")

    loads = [
        pltpu.make_async_copy(sky_h, sky, isem.at[0]),
        pltpu.make_async_copy(obs_h, obs, isem.at[1]),
        pltpu.make_async_copy(wts_h, wts, isem.at[2]),
    ]
    for cp in loads:
        cp.start()

    barrier = pltpu.get_barrier_semaphore()
    for k in range(1, NF):
        pl.semaphore_signal(barrier, inc=1, device_id={"facet": lax.rem(f + k, NF)}, device_id_type=MESH)
    for k in range(1, NC):
        pl.semaphore_signal(barrier, inc=1, device_id={"col": lax.rem(c + k, NC)}, device_id_type=MESH)

    def begin(phase, send, recv, axis, n, me):
        copies = []
        for k in range(1, n):
            peer = lax.rem(me + k, n)
            cp = pltpu.make_async_remote_copy(
                src_ref=send.at[peer],
                dst_ref=recv.at[me],
                send_sem=ssem.at[phase, k],
                recv_sem=rsem.at[phase, k],
                device_id={axis: peer},
                device_id_type=MESH,
            )
            cp.start()
            copies.append(cp)
        recv[me] = send[me]
        return copies

    s_me = offs[f, 0]
    t_me = offs[f, 1]
    lane = iota((1, 128), 1)
    low = lane < 64
    part = (lane >> 5) & 1

    l256 = iota((1, LJ), 1)
    cv = 8 * (l256 & 31)
    for b in range(NC):
        cv = cv + jnp.where((l256 >> 5) == b, cols[b], 0)
    bc, bs = turns(iota((LJ, LJ), 0) * cv, 16, 1.0)
    bm[0:256, 0:256] = bc
    bm[0:256, 256:512] = -bs
    bm[256:512, 0:256] = bs
    bm[256:512, 256:512] = bc
    ac, as_ = turns((t_me * FN + LJ * iota((NI, LJ), 0)) * cv, 16, 1.0 / math.sqrt(FN))
    at[0] = ac
    at[1] = as_

    def columns_forward(image, send):
        x = [
            jnp.concatenate([image[d, :, LJ * i:LJ * (i + 1)] for i in range(NI)], axis=0)
            for d in range(2)
        ]
        zs[...] = dot(jnp.concatenate(x, axis=1), bm[...])
        re = jnp.zeros((SLAB, LJ), F32)
        im = jnp.zeros((SLAB, LJ), F32)
        for i in range(NI):
            zr = zs[SLAB * i:SLAB * (i + 1), 0:256]
            zi = zs[SLAB * i:SLAB * (i + 1), 256:512]
            wc = at[0, i:i + 1, :]
            ws = at[1, i:i + 1, :]
            re = re + (wc * zr + ws * zi)
            im = im + (wc * zi - ws * zr)
        for g in range(2):
            rot_re = [re[:, 128 * g:128 * g + 128]]
            rot_im = [im[:, 128 * g:128 * g + 128]]
            for m in range(1, 4):
                rot_re.append(pltpu.roll(rot_re[0], 32 * m, 1))
                rot_im.append(pltpu.roll(rot_im[0], 32 * m, 1))
            for k in range(4):
                send[4 * g + k] = jnp.where(
                    low,
                    jnp.where(part == 0, rot_re[(4 - k) % 4], rot_im[(5 - k) % 4]),
                    jnp.where(part == 0, rot_re[(6 - k) % 4], rot_im[(7 - k) % 4]),
                )

    def rows_forward(recv, send):
        x = recv[...].reshape(FROWS, 128)
        y = pltpu.roll(x, 32, 1)
        y = jnp.where(part == 0, y, -y)
        out = dot(vt[...], jnp.concatenate([x, y], axis=0))
        send[...] = jnp.where(low, out[0:256], out[256:512]).reshape(NF, SLAB, 128)

    def model(recv):
        x = recv[...].reshape(256, 128)
        for h in range(2):
            zs[256 * h:256 * (h + 1), :] = dot(x, wz[128 * h:128 * (h + 1), :])
        for h in range(2):
            for a in range(NF):
                r0 = 256 * h + SLAB * a
                zr = zs[r0:r0 + SLAB, 0:256]
                zi = zs[r0:r0 + SLAB, 256:512]
                wc = tf[0, a:a + 1, :]
                ws = tf[1, a:a + 1, :]
                vr = wc * zr + ws * zi
                vi = wc * zi - ws * zr
                tt[r0:r0 + SLAB, 0:256] = vr
                tt[r0:r0 + SLAB, 256:512] = vi
                tt[512 + r0:512 + r0 + SLAB, 0:256] = vi
                tt[512 + r0:512 + r0 + SLAB, 256:512] = -vr
        return dot(pt[...], tt[...])

    loads[0].wait()
    columns_forward(sky, send1)
    pl.semaphore_wait(barrier, NF - 1 + NC - 1)
    sent = begin(0, send1, recv1, "col", NC, c)

    p16 = iota((SLAB, 128), 0)
    r128 = s_me * FN + iota((SLAB, 128), 1)
    vscale = 1.0 / math.sqrt(FROWS)
    for h in range(2):
        for a in range(NF):
            vc, vs = turns(r128 * (rows[a] + 512 * (SLAB * h + p16)), 16, vscale)
            r0 = 256 * h + SLAB * a
            vt[r0:r0 + SLAB, 0:128] = vc
            vt[r0:r0 + SLAB, 128:256] = vs
    for cp in sent:
        cp.wait_recv()
    rows_forward(recv1, send2)
    sent2 = begin(1, send2, recv2, "facet", NF, f)

    c16, s16 = turns(iota((M, G), 0) * iota((M, G), 1), 8, 1.0 / 16)
    zero = jnp.zeros((64, 512), F32)
    for h in range(2):
        r0 = 128 * h + 64 * h
        wz[r0:r0 + 32, 0:256] = c16
        wz[r0:r0 + 32, 256:512] = -s16
        wz[r0 + 32:r0 + 64, 0:256] = s16
        wz[r0 + 32:r0 + 64, 256:512] = c16
        z0 = 128 * h + 64 * (1 - h)
        wz[z0:z0 + 64, :] = zero
    tv = jnp.zeros((NF, G), jnp.int32)
    i16 = iota((NF, G), 0)
    for a in range(NF):
        tv = jnp.where(i16 == a, offs[a, 1], tv)
    tc, ts = turns(tv * iota((NF, G), 1), 3, 1.0)
    tf[0] = tc
    tf[1] = ts
    l512 = iota((1, 512), 1)
    place = (l512 & 15) + SLAB * (l512 >> 8)
    for a in range(NF):
        place = place + jnp.where(((l512 >> 4) & 15) == a, offs[a, 0] * M, 0)
    pc, ps_ = turns(iota((G, 512), 0) * place, 8, 1.0 / 16)
    pt[:, 0:512] = pc
    pt[:, 512:1024] = ps_
    u256 = iota((SLAB, G), 1)
    q16 = iota((SLAB, G), 0)
    for h in range(2):
        for a in range(NF):
            kc, ks = turns((offs[a, 0] * M + SLAB * h + q16) * u256, 8, 1.0 / 16)
            r0 = 256 * h + SLAB * a
            pk[r0:r0 + SLAB, 0:256] = kc
            pk[r0:r0 + SLAB, 256:512] = ks
    wc_, ws_ = turns(iota((G, 128), 0) * (lane & 31), 8, 1.0 / 16)
    wt[0:256, :] = jnp.where(part == 0, wc_, ws_)
    wt[256:512, :] = jnp.where(part == 0, -ws_, wc_)
    loads[1].wait()
    loads[2].wait()
    for cp in sent2:
        cp.wait_recv()

    first = model(recv2)
    mask = wts[...].astype(F32)
    rre = mask * (obs[0] - first[:, 0:256])
    rim = mask * (obs[1] - first[:, 256:512])
    rr[0:256, 0:256] = rre
    rr[0:256, 256:512] = rim
    rr[256:512, 0:256] = -rim
    rr[256:512, 256:512] = rre
    zs[...] = dot(pk[...], rr[...])
    for h in range(2):
        for a in range(NF):
            r0 = 256 * h + SLAB * a
            zr = zs[r0:r0 + SLAB, 0:256]
            zi = zs[r0:r0 + SLAB, 256:512]
            wc = tf[0, a:a + 1, :]
            ws = tf[1, a:a + 1, :]
            uu[r0:r0 + SLAB, 0:256] = wc * zr - ws * zi
            uu[r0:r0 + SLAB, 256:512] = wc * zi + ws * zr
    out = dot(uu[...], wt[...])
    send3[...] = jnp.where(low, out[0:256], out[256:512]).reshape(NF, SLAB, 128)
    sent3 = begin(2, send3, recv3, "facet", NF, f)

    fl = 512 * (l256 & 15)
    for a in range(NF):
        fl = fl + jnp.where((l256 >> 4) == a, rows[a], 0)
    rcol = s_me * FN + iota((FROWS, LJ), 0)
    for h in range(2):
        vc, vs = turns(rcol * (fl + 512 * SLAB * h), 16, vscale)
        vb[128 * h:128 * h + 128, :] = vc
        vb[256 + 128 * h:256 + 128 * h + 128, :] = vs
    j256 = iota((M, LJ), 1)
    q32 = iota((M, LJ), 0)
    for b in range(NC):
        bc, bs = turns(j256 * (cols[b] + 8 * q32), 16, 1.0)
        bt[32 * b:32 * b + 32, 0:256] = bc
        bt[32 * b:32 * b + 32, 256:512] = bs
        bt[256 + 32 * b:256 + 32 * b + 32, 0:256] = -bs
        bt[256 + 32 * b:256 + 32 * b + 32, 256:512] = bc
    for cp in sent3:
        cp.wait_recv()

    out = dot(vb[...], recv3[...].reshape(256, 128))
    dd = jnp.where(low, out[0:128], out[128:256])
    ee = jnp.where(low, out[256:384], out[384:512])
    dd = dd + pltpu.roll(dd, 64, 1)
    ee = ee + pltpu.roll(ee, 64, 1)
    ee = pltpu.roll(ee, 32, 1)
    send4[...] = (dd + jnp.where(part == 0, -ee, ee)).reshape(NC, SLAB, 128)
    sent4 = begin(3, send4, recv4, "col", NC, c)
    for cp in sent4:
        cp.wait_recv()

    tiles_re = []
    tiles_im = []
    for g in range(2):
        a = [recv4[4 * g + k] for k in range(4)]
        w = [pltpu.roll(v, 32, 1) for v in a]
        tiles_re.append(
            jnp.where(low, jnp.where(part == 0, a[0], w[1]), jnp.where(part == 0, a[2], w[3]))
        )
        tiles_im.append(
            jnp.where(low, jnp.where(part == 0, w[0], a[1]), jnp.where(part == 0, w[2], a[3]))
        )
    sre = jnp.concatenate(tiles_re, axis=1)
    sim = jnp.concatenate(tiles_im, axis=1)
    for i in range(NI):
        wc = at[0, i:i + 1, :]
        ws = at[1, i:i + 1, :]
        uu[SLAB * i:SLAB * (i + 1), 0:256] = sre * wc - sim * ws
        uu[SLAB * i:SLAB * (i + 1), 256:512] = sim * wc + sre * ws
    zs[...] = dot(uu[...], bt[...])
    for i in range(NI):
        ur = sky[0, :, LJ * i:LJ * (i + 1)] + zs[SLAB * i:SLAB * (i + 1), 0:256]
        ui = sky[1, :, LJ * i:LJ * (i + 1)] + zs[SLAB * i:SLAB * (i + 1), 256:512]
        mag = jnp.sqrt(ur * ur + ui * ui)
        ratio = jnp.maximum(mag - SHRINK, 0.0) / jnp.maximum(mag, SHRINK)
        new[0, :, LJ * i:LJ * (i + 1)] = ur * ratio
        new[1, :, LJ * i:LJ * (i + 1)] = ui * ratio
    store_new = pltpu.make_async_copy(new, new_h, osem.at[0])
    store_new.start()

    columns_forward(new, send5)
    sent5 = begin(4, send5, recv5, "col", NC, c)
    for cp in sent5:
        cp.wait_recv()
    rows_forward(recv5, send6)
    sent6 = begin(5, send6, recv6, "facet", NF, f)
    for cp in sent6:
        cp.wait_recv()
    second = model(recv6)
    pred[0] = second[:, 0:256]
    pred[1] = second[:, 256:512]
    store_pred = pltpu.make_async_copy(pred, pred_h, osem.at[1])
    store_pred.start()
    for group in (sent, sent2, sent3, sent4, sent5, sent6):
        for cp in group:
            cp.wait_send()
    store_new.wait()
    store_pred.wait()


def local(sky_image, observed, weights, facet_offsets, subgrid_rows, subgrid_columns):
    smem = pl.BlockSpec(memory_space=pltpu.SMEM)
    hbm = pl.BlockSpec(memory_space=pl.ANY)
    small = pltpu.VMEM((NC, SLAB, 128), F32)
    large = pltpu.VMEM((NF, SLAB, 128), F32)
    square = pltpu.VMEM((512, 512), F32)
    return pl.pallas_call(
        kernel,
        out_shape=(
            jax.ShapeDtypeStruct((2, SLAB, FN), F32),
            jax.ShapeDtypeStruct((2, G, G), F32),
        ),
        in_specs=[smem, smem, smem, hbm, hbm, hbm],
        out_specs=(hbm, hbm),
        scratch_shapes=[
            pltpu.VMEM((2, SLAB, FN), F32),
            pltpu.VMEM((2, G, G), F32),
            pltpu.VMEM((G, G), jnp.int32),
            pltpu.VMEM((2, SLAB, FN), F32),
            pltpu.VMEM((2, G, G), F32),
            square,
            square,
            pltpu.VMEM((2, NI, LJ), F32),
            pltpu.VMEM((512, 256), F32),
            pltpu.VMEM((512, 256), F32),
            pltpu.VMEM((256, 512), F32),
            pltpu.VMEM((512, 128), F32),
            pltpu.VMEM((2, NF, G), F32),
            pltpu.VMEM((256, 1024), F32),
            square,
            square,
            pltpu.VMEM((1024, 512), F32),
            square,
            square,
            small, small, large, large, large, large, small, small, small, small, large, large,
            pltpu.SemaphoreType.DMA((6, NF)),
            pltpu.SemaphoreType.DMA((6, NF)),
            pltpu.SemaphoreType.DMA((3,)),
            pltpu.SemaphoreType.DMA((2,)),
        ],
        compiler_params=pltpu.CompilerParams(
            collective_id=0, has_side_effects=True, vmem_limit_bytes=40 * 1024 * 1024
        ),
        name="imaging",
    )(facet_offsets, subgrid_rows, subgrid_columns, sky_image, observed, weights)


def solution(mesh):
    return jax.shard_map(
        local,
        mesh=mesh,
        in_specs=(
            P(None, ("facet", "col"), None),
            P(None, "facet", "col"),
            P("facet", "col"),
            P(),
            P(),
            P(),
        ),
        out_specs=(P(None, ("facet", "col"), None), P(None, "facet", "col")),
        check_vma=False,
    )
```

```python
import math

import jax
import jax.numpy as jnp
from jax import lax
from jax.experimental import pallas as pl
from jax.experimental.pallas import tpu as pltpu
from jax.sharding import PartitionSpec as P

FN = 8192
M = 32
SLOTS = 8
NIMG = 65536
G = 256
FROWS = 128
NF = 16
NC = 8
SLAB = 16
LJ = 256
NI = 32
SHRINK = 0.5
F32 = jnp.float32
BF16 = jnp.bfloat16
MESH = pl.DeviceIdType.MESH


def iota(shape, dim):
    return lax.broadcasted_iota(jnp.int32, shape, dim)


def turns(k, bits, scale):
    n = 1 << bits
    k = k & (n - 1)
    q = (k + n // 8) >> (bits - 2)
    x = (k - (q << (bits - 2))).astype(F32) * (2.0 * math.pi / n)
    y = x * x
    s = x * (1.0 + y * (-1.0 / 6 + y * (1.0 / 120 + y * (-1.0 / 5040 + y * (1.0 / 362880)))))
    c = 1.0 + y * (-0.5 + y * (1.0 / 24 + y * (-1.0 / 720 + y * (1.0 / 40320 + y * (-1.0 / 3628800)))))
    swap = (q & 1) == 1
    cc = jnp.where(swap, s, c) * scale
    ss = jnp.where(swap, c, s) * scale
    return (
        jnp.where(((q + 1) & 2) != 0, -cc, cc),
        jnp.where((q & 2) != 0, -ss, ss),
    )


def split(x):
    high = x.astype(BF16)
    return high, (x - high.astype(F32)).astype(BF16)


def put_left(ref, rows, start, x):
    high, rest = split(x)
    k = ref.shape[-1] // 3
    n = x.shape[1]
    ref[rows, start:start + n] = high
    ref[rows, k + start:k + start + n] = rest
    ref[rows, 2 * k + start:2 * k + start + n] = high


def put_right(ref, start, columns, x):
    high, rest = split(x)
    k = ref.shape[-2] // 3
    n = x.shape[0]
    ref[start:start + n, columns] = high
    ref[k + start:k + start + n, columns] = high
    ref[2 * k + start:2 * k + start + n, columns] = rest


def right(x):
    high, rest = split(x)
    return jnp.concatenate([high, high, rest], axis=0)


def dot(a, b):
    return lax.dot_general(a, b, (((1,), (0,)), ((), ())), preferred_element_type=F32)


def span(start, size):
    return slice(start, start + size)


ALL = slice(None)
COL_STEPS = ((1, 2), (1, 1), (1, 3), (0, 2), (1, 0), (0, 1), (0, 3))
FACET_STEPS = tuple(
    sorted(
        ((y, x, k) for y in range(4) for x in range(2) for k in range(2) if y + x + k > 0),
        key=lambda d: -(min(d[0], 4 - d[0]) + d[1]),
    )
)


def lanes():
    lane = iota((1, 128), 1)
    return lane < 64, (lane >> 5) & 1


def model(parts, wz, tf, pt, zs, tt):
    low, _ = lanes()
    x = parts[...].reshape(256, 128)
    high = x.astype(BF16).astype(F32)
    rest = x - high
    a = jnp.concatenate(
        [
            jnp.where(low, high, pltpu.roll(rest, 64, 1)),
            jnp.where(low, pltpu.roll(high, 64, 1), rest),
        ],
        axis=0,
    ).astype(BF16)
    zs[...] = dot(jnp.concatenate([a, a], axis=1), wz[...])
    sums = []
    for h in range(2):
        for k in range(NF):
            rows = span(256 * h + SLAB * k, SLAB)
            zr = zs[rows, 0:256]
            zi = zs[rows, 256:512]
            wc = tf[0, k:k + 1, :]
            ws = tf[1, k:k + 1, :]
            put_right(tt.at[h], SLAB * k, span(0, 256), wc * zr + ws * zi)
            put_right(tt.at[h], SLAB * k, span(256, 256), wc * zi - ws * zr)
        g = dot(pt[span(256 * h, 256), :], tt[h])
        sums.append((g[0:128, 0:256] + g[128:256, 256:512], g[0:128, 256:512] - g[128:256, 0:256]))
    (er, ei), (odd_r, odd_i) = sums
    return (er + odd_r, ei + odd_i), (er - odd_r, ei - odd_i)


def finish_kernel(parts, wz, tf, pt, new, new_h, pred_h, pred, zs, tt, sem):
    store_new = pltpu.make_async_copy(new, new_h, sem.at[0])
    store_new.start()
    stores = [store_new]
    for half, values in enumerate(model(parts, wz, tf, pt, zs, tt)):
        for d in range(2):
            rows = span(128 * half, 128)
            pred[d, rows, :] = values[d]
            cp = pltpu.make_async_copy(pred.at[d, rows, :], pred_h.at[d, rows, :], sem.at[1 + 2 * half + d])
            cp.start()
            stores.append(cp)
    for cp in stores:
        cp.wait()


def kernel(
    offs_h, rows_h, cols_h, sky_h, obs_h, wts_h,
    recv6, wz, tf, pt, new,
    offs, rows, cols, sky, obs, wts,
    bm, bt, at, vt, vb, wt, pk, zs, tt, rt, uu,
    send1, recv1, send2, recv2, send3, recv3, send4, recv4, send5, recv5, send6,
    ssem, rsem, isem,
):
    f = lax.axis_index("facet")
    c = lax.axis_index("col")

    loads = [
        pltpu.make_async_copy(src, dst, isem.at[n])
        for n, (src, dst) in enumerate(
            ((cols_h, cols), (offs_h, offs), (rows_h, rows), (sky_h, sky), (obs_h, obs), (wts_h, wts))
        )
    ]
    for cp in loads:
        cp.start()

    fy, fx, fk = lax.div(f, 4), lax.rem(lax.div(f, 2), 2), lax.rem(f, 2)
    cx, cz = lax.div(c, 4), lax.rem(c, 4)
    col_peers = [4 * lax.rem(cx + x, 2) + lax.rem(cz + z, 4) for x, z in COL_STEPS]
    facet_peers = [
        4 * lax.rem(fy + y, 4) + 2 * lax.rem(fx + x, 2) + lax.rem(fk + k, 2) for y, x, k in FACET_STEPS
    ]
    barrier = pltpu.get_barrier_semaphore()
    for peer in facet_peers:
        pl.semaphore_signal(barrier, inc=1, device_id={"facet": peer}, device_id_type=MESH)
    for peer in col_peers:
        pl.semaphore_signal(barrier, inc=1, device_id={"col": peer}, device_id_type=MESH)

    def start(phase, send, recv, axis):
        me, peers = (c, col_peers) if axis == "col" else (f, facet_peers)

        def copy(src, dst, peer):
            return pltpu.make_async_remote_copy(
                src_ref=src, dst_ref=dst, send_sem=ssem.at[phase], recv_sem=rsem.at[phase],
                device_id={axis: peer}, device_id_type=MESH,
            )

        for peer in peers:
            copy(send.at[peer], recv.at[me], peer).start()
        recv[me] = send[me]
        n = len(peers)
        return copy(send.at[pl.ds(0, n)], recv.at[pl.ds(0, n)], peers[0])

    low, part = lanes()
    lane = iota((1, 128), 1)

    def unpack(x):
        y = pltpu.roll(x, 64, 1)
        return jnp.where(low, x, y), jnp.where(low, y, x)

    l256 = iota((1, LJ), 1)
    cv = 8 * (l256 & 31)
    loads[0].wait()
    for b in range(NC):
        cv = cv + jnp.where((l256 >> 5) == b, cols[b], 0)
    bc, bs = turns(iota((LJ, LJ), 0) * cv, 16, 1.0)
    put_right(bm, 0, span(0, 256), bc)
    put_right(bm, 0, span(256, 256), -bs)
    put_right(bm, 256, span(0, 256), bs)
    put_right(bm, 256, span(256, 256), bc)
    loads[1].wait()
    s_me = offs[0, f]
    t_me = offs[1, f]
    ac, as_ = turns((t_me * FN + LJ * iota((NI, LJ), 0)) * cv, 16, 1.0 / math.sqrt(FN))
    at[0] = ac
    at[1] = as_

    def columns_forward(image, send):
        for i in range(NI):
            for d in range(2):
                put_left(uu, span(SLAB * i, SLAB), 256 * d, image[d, :, LJ * i:LJ * (i + 1)])
        zs[...] = dot(uu[...], bm[...])
        re = jnp.zeros((SLAB, LJ), F32)
        im = jnp.zeros((SLAB, LJ), F32)
        for i in range(NI):
            zr = zs[SLAB * i:SLAB * (i + 1), 0:256]
            zi = zs[SLAB * i:SLAB * (i + 1), 256:512]
            wc = at[0, i:i + 1, :]
            ws = at[1, i:i + 1, :]
            re = re + (wc * zr + ws * zi)
            im = im + (wc * zi - ws * zr)
        for g in range(2):
            rot_re = [re[:, 128 * g:128 * g + 128]]
            rot_im = [im[:, 128 * g:128 * g + 128]]
            for m in range(1, 4):
                rot_re.append(pltpu.roll(rot_re[0], 32 * m, 1))
                rot_im.append(pltpu.roll(rot_im[0], 32 * m, 1))
            for k in range(4):
                send[4 * g + k] = jnp.where(
                    low,
                    jnp.where(part == 0, rot_re[(4 - k) % 4][0:8], rot_im[(5 - k) % 4][0:8]),
                    jnp.where(part == 0, rot_re[(6 - k) % 4][8:16], rot_im[(7 - k) % 4][8:16]),
                )

    def rows_forward(recv, send):
        x = jnp.concatenate(unpack(recv[...].reshape(64, 128)), axis=0)
        y = pltpu.roll(x, 32, 1)
        y = jnp.where(part == 0, y, -y)
        out = dot(vt[...], right(jnp.concatenate([x, y], axis=0)))
        send[...] = jnp.where(low, out[0:256], out[256:512]).reshape(NF, SLAB, 128)

    loads[3].wait()
    columns_forward(sky, send1)
    pl.semaphore_wait(barrier, NF - 1 + NC - 1)
    wait1 = start(0, send1, recv1, "col")

    loads[2].wait()
    p16 = iota((SLAB, 128), 0)
    l128 = iota((SLAB, 128), 1)
    r128 = s_me * FN + SLAB * ((l128 >> 3) & 7) + 8 * (l128 >> 6) + (l128 & 7)
    vscale = 1.0 / math.sqrt(FROWS)
    for h in range(2):
        for a in range(NF):
            vc, vs = turns(r128 * (rows[a] + 512 * (2 * p16 + h)), 16, vscale)
            put_left(vt, span(256 * h + SLAB * a, SLAB), 0, vc)
            put_left(vt, span(256 * h + SLAB * a, SLAB), 128, vs)
    wait1.wait_recv()
    rows_forward(recv1, send2)
    wait2 = start(1, send2, recv2, "facet")

    for d in range(0, M, SLAB):
        wc, ws = turns((d + iota((SLAB, G), 0)) * iota((SLAB, G), 1), 8, 1.0 / 16)
        for r0, n, x in ((d, 0, wc), (d, 256, -ws), (M + d, 0, ws), (M + d, 256, wc)):
            high, rest = split(x)
            wz[r0:r0 + SLAB, n:n + 256] = high
            wz[64 + r0:64 + r0 + SLAB, n:n + 256] = high
            wz[128 + r0:128 + r0 + SLAB, n:n + 256] = rest
    wz[192:256, :] = jnp.zeros((64, 512), BF16)
    tv = jnp.zeros((NF, G), jnp.int32)
    i16 = iota((NF, G), 0)
    for a in range(NF):
        tv = jnp.where(i16 == a, offs[1, a], tv)
    tc, ts = turns(tv * iota((NF, G), 1), 3, 1.0)
    tf[0] = tc
    tf[1] = ts
    place = 2 * (l256 & 15)
    for a in range(NF):
        place = place + jnp.where((l256 >> 4) == a, offs[0, a] * M, 0)
    for h in range(2):
        pc, ps_ = turns(iota((128, 256), 0) * (place + h), 8, 1.0 / 16)
        put_left(pt, span(256 * h, 128), 0, pc)
        put_left(pt, span(256 * h + 128, 128), 0, ps_)
    for h in range(2):
        for a in range(NF):
            kc, ks = turns((offs[0, a] * M + h + 2 * p16) * l128, 8, 1.0 / 16)
            put_left(pk, span(256 * h + SLAB * a, SLAB), 0, kc)
            put_left(pk, span(256 * h + SLAB * a, SLAB), 128, ks)
    wc_, ws_ = turns(iota((G, 128), 0) * (lane & 31), 8, 1.0 / 16)
    put_right(wt, 0, ALL, jnp.where(part == 0, wc_, ws_))
    put_right(wt, 256, ALL, jnp.where(part == 0, -ws_, wc_))
    loads[4].wait()
    loads[5].wait()
    wait2.wait_recv()

    resid = []
    for half, (mr, mi) in enumerate(model(recv2, wz, tf, pt, zs, tt)):
        rs = span(128 * half, 128)
        mask = wts[rs, :].astype(F32)
        resid.append((mask * (obs[0, rs, :] - mr), mask * (obs[1, rs, :] - mi)))
    outs = []
    for h in range(2):
        rr, ri = [
            resid[0][d] + resid[1][d] if h == 0 else resid[0][d] - resid[1][d] for d in range(2)
        ]
        put_right(rt.at[h], 0, span(0, 256), rr)
        put_right(rt.at[h], 0, span(256, 256), ri)
        put_right(rt.at[h], 128, span(0, 256), -ri)
        put_right(rt.at[h], 128, span(256, 256), rr)
        zs[span(256 * h, 256), :] = dot(pk[span(256 * h, 256), :], rt[h])
        for a in range(NF):
            zr = zs[span(256 * h + SLAB * a, SLAB), 0:256]
            zi = zs[span(256 * h + SLAB * a, SLAB), 256:512]
            wc = tf[0, a:a + 1, :]
            ws = tf[1, a:a + 1, :]
            put_left(uu, span(256 * h + SLAB * a, SLAB), 0, wc * zr - ws * zi)
            put_left(uu, span(256 * h + SLAB * a, SLAB), 256, wc * zi + ws * zr)
        outs.append(dot(uu[span(256 * h, 256), :], wt[...]))
    send3[...] = jnp.where(low, outs[0], outs[1]).reshape(NF, SLAB, 128)
    wait3 = start(2, send3, recv3, "facet")

    fl = 1024 * (l256 & 15)
    for a in range(NF):
        fl = fl + jnp.where((l256 >> 4) == a, rows[a], 0)
    r0 = iota((FROWS, LJ), 0)
    rcol = s_me * FN + SLAB * ((r0 >> 3) & 7) + 8 * (r0 >> 6) + (r0 & 7)
    for h in range(2):
        vc, vs = turns(rcol * (fl + 512 * h), 16, vscale)
        put_left(vb, span(128 * h, 128), 0, vc)
        put_left(vb, span(256 + 128 * h, 128), 0, vs)
    j256 = iota((M, LJ), 1)
    q32 = iota((M, LJ), 0)
    for b in range(NC):
        bc, bs = turns(j256 * (cols[b] + 8 * q32), 16, 1.0)
        put_right(bt, 32 * b, span(0, 256), bc)
        put_right(bt, 32 * b, span(256, 256), bs)
        put_right(bt, 256 + 32 * b, span(0, 256), -bs)
        put_right(bt, 256 + 32 * b, span(256, 256), bc)
    wait3.wait_recv()

    out = dot(vb[...], right(recv3[...].reshape(256, 128)))
    dd = jnp.where(low, out[0:128], out[128:256])
    ee = jnp.where(low, out[256:384], out[384:512])
    dd = dd + pltpu.roll(dd, 64, 1)
    ee = ee + pltpu.roll(ee, 64, 1)
    ee = pltpu.roll(ee, 32, 1)
    dd = dd + jnp.where(part == 0, -ee, ee)
    send4[...] = jnp.where(low, dd[0:64], dd[64:128]).reshape(NC, 8, 128)
    wait4 = start(3, send4, recv4, "col")
    wait4.wait_recv()

    x4 = jnp.concatenate(unpack(recv4[...].reshape(64, 128)), axis=0)
    y4 = pltpu.roll(x4, 32, 1)
    tiles = []
    for d in range(2):
        halves = []
        for half in range(2):
            row = []
            for g in range(2):
                a = []
                for k in range(4):
                    src = x4 if (k + d) % 2 == 0 else y4
                    r0 = 64 * half + 8 * (4 * g + k)
                    a.append(src[r0:r0 + 8])
                row.append(
                    jnp.where(low, jnp.where(part == 0, a[0], a[1]), jnp.where(part == 0, a[2], a[3]))
                )
            halves.append(jnp.concatenate(row, axis=1))
        tiles.append(jnp.concatenate(halves, axis=0))
    sre, sim = tiles
    for i in range(NI):
        wc = at[0, i:i + 1, :]
        ws = at[1, i:i + 1, :]
        put_left(uu, span(SLAB * i, SLAB), 0, sre * wc - sim * ws)
        put_left(uu, span(SLAB * i, SLAB), 256, sim * wc + sre * ws)
    zs[...] = dot(uu[...], bt[...])
    for i in range(NI):
        ur = sky[0, :, LJ * i:LJ * (i + 1)] + zs[SLAB * i:SLAB * (i + 1), 0:256]
        ui = sky[1, :, LJ * i:LJ * (i + 1)] + zs[SLAB * i:SLAB * (i + 1), 256:512]
        mag = jnp.sqrt(ur * ur + ui * ui)
        ratio = jnp.maximum(mag - SHRINK, 0.0) / jnp.maximum(mag, SHRINK)
        new[0, :, LJ * i:LJ * (i + 1)] = ur * ratio
        new[1, :, LJ * i:LJ * (i + 1)] = ui * ratio

    columns_forward(new, send5)
    wait5 = start(4, send5, recv5, "col")
    wait5.wait_recv()
    rows_forward(recv5, send6)
    wait6 = start(5, send6, recv6, "facet")
    wait6.wait_recv()
    for wait in (wait1, wait2, wait3, wait4, wait5, wait6):
        wait.wait_send()


def local(sky_image, observed, weights, facet_offsets, subgrid_rows, subgrid_columns):
    vmem = pl.BlockSpec(memory_space=pltpu.VMEM)
    hbm = pl.BlockSpec(memory_space=pltpu.HBM)
    small = pltpu.VMEM((NC, 8, 128), F32)
    large = pltpu.VMEM((NF, SLAB, 128), F32)

    def left(rows, columns):
        return pltpu.VMEM((rows, 3 * columns), BF16)

    def right_of(rows, columns):
        return pltpu.VMEM((3 * rows, columns), BF16)

    operands = [
        pltpu.with_memory_space_constraint(x, pltpu.HBM)
        for x in (facet_offsets.T, subgrid_rows, subgrid_columns, sky_image, observed, weights)
    ]
    halfway = pltpu.VMEM((512, 512), F32)
    stack = pltpu.VMEM((2, 768, 512), BF16)
    parts, wz, tf, pt, new = pl.pallas_call(
        kernel,
        out_shape=(
            pltpu.VMEM((NF, SLAB, 128), F32),
            pltpu.VMEM((256, 512), BF16),
            pltpu.VMEM((2, NF, G), F32),
            pltpu.VMEM((512, 768), BF16),
            pltpu.VMEM((2, SLAB, FN), F32),
        ),
        in_specs=[hbm] * 6,
        out_specs=(vmem,) * 5,
        scratch_shapes=[
            pltpu.SMEM((2, NF), jnp.int32),
            pltpu.SMEM((NF,), jnp.int32),
            pltpu.SMEM((NC,), jnp.int32),
            pltpu.VMEM((2, SLAB, FN), F32),
            pltpu.VMEM((2, G, G), F32),
            pltpu.VMEM((G, G), jnp.int32),
            right_of(512, 512),
            right_of(512, 512),
            pltpu.VMEM((2, NI, LJ), F32),
            left(512, 256),
            left(512, 256),
            right_of(512, 128),
            left(512, 256),
            halfway,
            stack,
            stack,
            left(512, 512),
            small, small, large, large, large, large, small, small, small, small, large,
            pltpu.SemaphoreType.DMA((6,)),
            pltpu.SemaphoreType.DMA((6,)),
            pltpu.SemaphoreType.DMA((6,)),
        ],
        compiler_params=pltpu.CompilerParams(
            collective_id=0, has_side_effects=True, vmem_limit_bytes=40 * 1024 * 1024
        ),
        name="imaging",
    )(*operands)
    return pl.pallas_call(
        finish_kernel,
        out_shape=(
            jax.ShapeDtypeStruct((2, SLAB, FN), F32),
            jax.ShapeDtypeStruct((2, G, G), F32),
        ),
        in_specs=[vmem] * 5,
        out_specs=(hbm, hbm),
        scratch_shapes=[
            pltpu.VMEM((2, G, G), F32),
            halfway,
            stack,
            pltpu.SemaphoreType.DMA((5,)),
        ],
        compiler_params=pltpu.CompilerParams(vmem_limit_bytes=32 * 1024 * 1024),
        name="finish",
    )(parts, wz, tf, pt, new)


def solution(mesh):
    return jax.shard_map(
        local,
        mesh=mesh,
        in_specs=(
            P(None, ("facet", "col"), None),
            P(None, "facet", "col"),
            P("facet", "col"),
            P(),
            P(),
            P(),
        ),
        out_specs=(P(None, ("facet", "col"), None), P(None, "facet", "col")),
        check_vma=False,
    )
```

```python
import math

import jax
import jax.numpy as jnp
from jax import lax
from jax.experimental import pallas as pl
from jax.experimental.pallas import tpu as pltpu
from jax.sharding import PartitionSpec as P

FN = 8192
M = 32
SLOTS = 8
NIMG = 65536
G = 256
FROWS = 128
NF = 16
NC = 8
SLAB = 16
LJ = 256
NI = 32
SHRINK = 0.5
F32 = jnp.float32
BF16 = jnp.bfloat16
MESH = pl.DeviceIdType.MESH


def iota(shape, dim):
    return lax.broadcasted_iota(jnp.int32, shape, dim)


def turns(k, bits, scale):
    n = 1 << bits
    k = k & (n - 1)
    q = (k + n // 8) >> (bits - 2)
    x = (k - (q << (bits - 2))).astype(F32) * (2.0 * math.pi / n)
    y = x * x
    s = x * (1.0 + y * (-1.0 / 6 + y * (1.0 / 120 + y * (-1.0 / 5040 + y * (1.0 / 362880)))))
    c = 1.0 + y * (-0.5 + y * (1.0 / 24 + y * (-1.0 / 720 + y * (1.0 / 40320 + y * (-1.0 / 3628800)))))
    swap = (q & 1) == 1
    cc = jnp.where(swap, s, c) * scale
    ss = jnp.where(swap, c, s) * scale
    return (
        jnp.where(((q + 1) & 2) != 0, -cc, cc),
        jnp.where((q & 2) != 0, -ss, ss),
    )


def split(x):
    high = x.astype(BF16)
    return high, (x - high.astype(F32)).astype(BF16)


def put_left(ref, rows, start, x):
    high, rest = split(x)
    k = ref.shape[-1] // 3
    n = x.shape[1]
    ref[rows, start:start + n] = high
    ref[rows, k + start:k + start + n] = rest
    ref[rows, 2 * k + start:2 * k + start + n] = high


def put_right(ref, start, columns, x):
    high, rest = split(x)
    k = ref.shape[-2] // 3
    n = x.shape[0]
    ref[start:start + n, columns] = high
    ref[k + start:k + start + n, columns] = high
    ref[2 * k + start:2 * k + start + n, columns] = rest


def right(x):
    high, rest = split(x)
    return jnp.concatenate([high, high, rest], axis=0)


def dot(a, b):
    return lax.dot_general(a, b, (((1,), (0,)), ((), ())), preferred_element_type=F32)


def span(start, size):
    return slice(start, start + size)


ALL = slice(None)
COL_STEPS = ((1, 2), (1, 1), (1, 3), (0, 2), (1, 0), (0, 1), (0, 3), (0, 0))
FACET_STEPS = (
    (2, 1, 0), (2, 1, 1), (2, 0, 0), (2, 0, 1), (1, 1, 0), (1, 1, 1), (3, 1, 0), (3, 1, 1),
    (1, 0, 0), (1, 0, 1), (3, 0, 0), (3, 0, 1), (0, 1, 0), (0, 1, 1), (0, 0, 1), (0, 0, 0),
)
COL_BACK = tuple(COL_STEPS.index((x, -z % 4)) for x, z in COL_STEPS)
FACET_BACK = tuple(FACET_STEPS.index((-y % 4, x, k)) for y, x, k in FACET_STEPS)
FACET_CROSS = tuple(FACET_STEPS.index((y, x, 1 - k)) for y, x, k in FACET_STEPS)
FACET_CROSS_BACK = tuple(FACET_STEPS.index((-y % 4, x, 1 - k)) for y, x, k in FACET_STEPS)
FAR, NEAR = 0, 1


def lanes():
    lane = iota((1, 128), 1)
    return lane < 64, (lane >> 5) & 1


def model_half(group, parts, wz, tf, pt, zs, tt):
    low, _ = lanes()
    x = parts.reshape(128, 128)
    high = x.astype(BF16).astype(F32)
    rest = x - high
    a = jnp.concatenate(
        [
            jnp.where(low, high, pltpu.roll(rest, 64, 1)),
            jnp.where(low, pltpu.roll(high, 64, 1), rest),
        ],
        axis=0,
    ).astype(BF16)
    zs[0:256, :] = dot(jnp.concatenate([a, a], axis=1), wz[...])
    sums = []
    for h in range(2):
        for k in range(8):
            rows = span(128 * h + SLAB * k, SLAB)
            zr = zs[rows, 0:256]
            zi = zs[rows, 256:512]
            wc = tf[0, 8 * group + k:8 * group + k + 1, :]
            ws = tf[1, 8 * group + k:8 * group + k + 1, :]
            put_right(tt.at[h], SLAB * k, span(0, 256), wc * zr + ws * zi)
            put_right(tt.at[h], SLAB * k, span(256, 256), wc * zi - ws * zr)
        sums.append(dot(pt[group, span(256 * h, 256), :], tt[h]))
    return sums


def combine(even, odd):
    (er, ei), (dr, di) = [
        (s[0:128, 0:256] + s[128:256, 256:512], s[0:128, 256:512] - s[128:256, 0:256])
        for s in (even, odd)
    ]
    return (er + dr, ei + di), (er - dr, ei - di)


def finish_kernel(parts, gs, wz, tf, pt, new, new_h, pred_h, pred, zs, tt, sem):
    store_new = pltpu.make_async_copy(new, new_h, sem.at[0])
    store_new.start()
    stores = [store_new]
    sums = model_half(FAR, parts[...], wz, tf, pt, zs, tt)
    for half, values in enumerate(combine(gs[0:256] + sums[0], gs[256:512] + sums[1])):
        for d in range(2):
            rows = span(128 * half, 128)
            pred[d, rows, :] = values[d]
            cp = pltpu.make_async_copy(pred.at[d, rows, :], pred_h.at[d, rows, :], sem.at[1 + 2 * half + d])
            cp.start()
            stores.append(cp)
    for cp in stores:
        cp.wait()


def kernel(
    offs_h, rows_h, cols_h, sky_h, obs_h, wts_h,
    parts, gs, wz, tf, pt, new,
    offs, rows, cols, sky, obs, wts,
    bm, bt, at, vt, vb, wt, pk, zs, tt, rt, uu, ud,
    send1, recv1, send2, recv2, send3, recv3, send4, recv4, send5, recv5, send6, recv6,
    ssem, rsem, isem,
):
    f = lax.axis_index("facet")
    c = lax.axis_index("col")

    loads = [
        pltpu.make_async_copy(src, dst, isem.at[n])
        for n, (src, dst) in enumerate(
            ((cols_h, cols), (offs_h, offs), (rows_h, rows), (sky_h, sky), (obs_h, obs), (wts_h, wts))
        )
    ]
    for cp in loads:
        cp.start()

    fy, fx, fk = lax.div(f, 4), lax.rem(lax.div(f, 2), 2), lax.rem(f, 2)
    cx, cz = lax.div(c, 4), lax.rem(c, 4)
    col_peers = [4 * lax.rem(cx + x, 2) + lax.rem(cz + z, 4) for x, z in COL_STEPS]
    facet_peers = [
        4 * lax.rem(fy + y, 4) + 2 * lax.rem(fx + x, 2) + lax.rem(fk + k, 2) for y, x, k in FACET_STEPS
    ]
    other = 4 * fy + 2 * fx + (1 - fk)
    barrier = pltpu.get_barrier_semaphore()
    for peer in facet_peers[:-1]:
        pl.semaphore_signal(barrier, inc=1, device_id={"facet": peer}, device_id_type=MESH)
    for peer in col_peers[:-1]:
        pl.semaphore_signal(barrier, inc=1, device_id={"facet": other, "col": peer}, device_id_type=MESH)

    def start(phase, group, send, recv, moves, own=None):
        def copy(src, dst, device):
            return pltpu.make_async_remote_copy(
                src_ref=src, dst_ref=dst, send_sem=ssem.at[phase, group], recv_sem=rsem.at[phase, group],
                device_id=device, device_id_type=MESH,
            )

        for block, slot, device in moves:
            copy(send.at[block], recv.at[slot], device).start()
        if own is not None:
            recv[own[1]] = send[own[0]]
        blocks = pl.ds(0, len(moves))
        return copy(send.at[blocks], recv.at[blocks], moves[0][2])

    def over_columns(phase, group, send, recv, cross=True):
        ks = range(4 * group, 4 * group + 4)
        if cross:
            moves = [(k, COL_BACK[k], {"facet": other, "col": col_peers[k]}) for k in ks]
            return start(phase, group, send, recv, moves)
        moves = [(k, COL_BACK[k], {"col": col_peers[k]}) for k in ks if k < NC - 1]
        return start(phase, group, send, recv, moves, (NC - 1, NC - 1) if group == NEAR else None)

    def to_subgrids(phase, group, send, recv, cross=True):
        back = FACET_CROSS_BACK if cross else FACET_BACK
        ks = range(8 * group, 8 * group + 8)
        moves = [(k, back[k], {"facet": facet_peers[k]}) for k in ks if k < NF - 1]
        return start(phase, group, send, recv, moves, (NF - 1, back[NF - 1]) if group == NEAR else None)

    def to_facets(phase, group, send, recv):
        moves, own = [], None
        for k in range(8 * group, 8 * group + 8):
            if FACET_CROSS[k] < NF - 1:
                moves.append((k, FACET_CROSS_BACK[k], {"facet": facet_peers[FACET_CROSS[k]]}))
            else:
                own = (k, FACET_CROSS_BACK[k])
        return start(phase, group, send, recv, moves, own)

    low, part = lanes()
    lane = iota((1, 128), 1)

    def unpack(x):
        y = pltpu.roll(x, 64, 1)
        return jnp.where(low, x, y), jnp.where(low, y, x)

    l256 = iota((1, LJ), 1)
    cv = 8 * (l256 & 31)
    loads[0].wait()
    for b in range(NC):
        cv = cv + jnp.where((l256 >> 5) == b, cols[col_peers[b]], 0)
    steps = iota((SLAB, LJ), 0)
    c1, s1 = turns((SLAB * steps) * cv, 16, 1.0)
    c0, s0 = turns(steps * cv, 16, 1.0)
    for k in range(SLAB):
        bc = c1[k:k + 1] * c0 - s1[k:k + 1] * s0
        bs = s1[k:k + 1] * c0 + c1[k:k + 1] * s0
        put_right(bm, SLAB * k, span(0, 256), bc)
        put_right(bm, SLAB * k, span(256, 256), -bs)
        put_right(bm, 256 + SLAB * k, span(0, 256), bs)
        put_right(bm, 256 + SLAB * k, span(256, 256), bc)
    loads[1].wait()
    s_me = offs[0, other]
    t_me = offs[1, f]
    ac, as_ = turns((t_me * FN + LJ * iota((NI, LJ), 0)) * cv, 16, 1.0 / math.sqrt(FN))
    at[0] = ac
    at[1] = as_

    def columns_forward(image, send, launch):
        for i in range(NI):
            for d in range(2):
                put_left(uu, span(SLAB * i, SLAB), 256 * d, image[d, :, LJ * i:LJ * (i + 1)])
        zs[...] = dot(uu[...], bm[...])
        re = jnp.zeros((SLAB, LJ), F32)
        im = jnp.zeros((SLAB, LJ), F32)
        for i in range(NI):
            zr = zs[span(SLAB * i, SLAB), 0:256]
            zi = zs[span(SLAB * i, SLAB), 256:512]
            wc = at[0, i:i + 1, :]
            ws = at[1, i:i + 1, :]
            re = re + (wc * zr + ws * zi)
            im = im + (wc * zi - ws * zr)
        for g in range(2):
            rot_re = [re[:, span(128 * g, 128)]]
            rot_im = [im[:, span(128 * g, 128)]]
            for m in range(1, 4):
                rot_re.append(pltpu.roll(rot_re[0], 32 * m, 1))
                rot_im.append(pltpu.roll(rot_im[0], 32 * m, 1))
            for k in range(4):
                send[4 * g + k] = jnp.where(
                    low,
                    jnp.where(part == 0, rot_re[(4 - k) % 4][0:8], rot_im[(5 - k) % 4][0:8]),
                    jnp.where(part == 0, rot_re[(6 - k) % 4][8:16], rot_im[(7 - k) % 4][8:16]),
                )
            launch(g)

    def row_products(vt, group, recv, targets):
        x = jnp.concatenate(unpack(recv[4 * group:4 * group + 4].reshape(32, 128)), axis=0)
        y = pltpu.roll(x, 32, 1)
        y = jnp.where(part == 0, y, -y)
        return dot(vt[group, targets, :], right(jnp.concatenate([x, y], axis=0)))

    def rows_forward(vt, waits, recv, phase, send, into, cross=True):
        waits[NEAR].wait_recv()
        near = row_products(vt, NEAR, recv, ALL)
        zs[:, 0:128] = near
        waits[FAR].wait_recv()
        later = []
        for g in range(2):
            out = zs[span(256 * g, 256), 0:128] + row_products(vt, FAR, recv, span(256 * g, 256))
            send[8 * g:8 * g + 8] = jnp.where(low, out[0:128], out[128:256]).reshape(8, SLAB, 128)
            later.append(to_subgrids(phase, g, send, into, cross))
        return later

    loads[3].wait()
    wait1 = []

    def launch1(g):
        if g == FAR:
            pl.semaphore_wait(barrier, NF - 1 + NC - 1)
        wait1.append(over_columns(0, g, send1, recv1))

    columns_forward(sky, send1, launch1)

    loads[2].wait()

    p16 = iota((SLAB, 128), 0)
    l128 = iota((SLAB, 128), 1)
    vscale = 1.0 / math.sqrt(FROWS)
    lane1 = lane & 63
    for g in range(2):
        slab = jnp.zeros((1, 128), jnp.int32)
        for k in range(4):
            slab = jnp.where(((lane1 >> 3) & 3) == k, col_peers[4 * g + k], slab)
        rlane = s_me * FN + SLAB * slab + 8 * (lane1 >> 5) + (lane1 & 7)
        for a in range(NF):
            for h in range(2):
                vc, vs = turns(rlane * (rows[facet_peers[a]] + 512 * (2 * p16 + h)), 16, vscale)
                r0 = 256 * (a // 8) + 128 * h + SLAB * (a % 8)
                put_left(vt.at[g], span(r0, SLAB), 0, jnp.where(low, vc, vs))
    wait2 = rows_forward(vt, wait1, recv1, 1, send2, recv2)

    for d in range(0, M, SLAB):
        wc, ws = turns((d + iota((SLAB, G), 0)) * iota((SLAB, G), 1), 8, 1.0 / 16)
        for r0, n, x in ((d, 0, wc), (d, 256, -ws), (M + d, 0, ws), (M + d, 256, wc)):
            high, rest = split(x)
            wz[r0:r0 + SLAB, n:n + 256] = high
            wz[64 + r0:64 + r0 + SLAB, n:n + 256] = high
            wz[128 + r0:128 + r0 + SLAB, n:n + 256] = rest
    wz[192:256, :] = jnp.zeros((64, 512), BF16)
    tv = jnp.zeros((NF, G), jnp.int32)
    i16 = iota((NF, G), 0)
    for a in range(NF):
        tv = jnp.where(i16 == a, offs[1, facet_peers[a]], tv)
    tc, ts = turns(tv * iota((NF, G), 1), 3, 1.0)
    tf[0] = tc
    tf[1] = ts
    for g in range(2):
        place = 2 * (lane & 15)
        for k in range(8):
            place = place + jnp.where((lane >> 4) == k, offs[0, facet_peers[8 * g + k]] * M, 0)
        for h in range(2):
            pc, ps_ = turns(iota((128, 128), 0) * (place + h), 8, 1.0 / 16)
            put_left(pt.at[g], span(256 * h, 128), 0, pc)
            put_left(pt.at[g], span(256 * h + 128, 128), 0, ps_)
    for h in range(2):
        for a in range(NF):
            kc, ks = turns((offs[0, facet_peers[a]] * M + h + 2 * p16) * l128, 8, 1.0 / 16)
            put_left(pk, span(256 * h + SLAB * a, SLAB), 0, kc)
            put_left(pk, span(256 * h + SLAB * a, SLAB), 128, ks)
    wc_, ws_ = turns(iota((G, 128), 0) * (lane & 31), 8, 1.0 / 16)
    put_right(wt, 0, ALL, jnp.where(part == 0, wc_, ws_))
    put_right(wt, 256, ALL, jnp.where(part == 0, -ws_, wc_))
    wait2[NEAR].wait_recv()
    for h, x in enumerate(model_half(NEAR, recv2[8:16], wz, tf, pt, zs, tt)):
        gs[span(256 * h, 256), :] = x
    loads[4].wait()
    loads[5].wait()
    wait2[FAR].wait_recv()

    sums = model_half(FAR, recv2[0:8], wz, tf, pt, zs, tt)
    resid = []
    for half, (mr, mi) in enumerate(combine(gs[0:256] + sums[0], gs[256:512] + sums[1])):
        rs = span(128 * half, 128)
        mask = wts[rs, :].astype(F32)
        resid.append((mask * (obs[0, rs, :] - mr), mask * (obs[1, rs, :] - mi)))
    for h in range(2):
        rr, ri = [
            resid[0][d] + resid[1][d] if h == 0 else resid[0][d] - resid[1][d] for d in range(2)
        ]
        put_right(rt.at[h], 0, span(0, 256), rr)
        put_right(rt.at[h], 0, span(256, 256), ri)
        put_right(rt.at[h], 128, span(0, 256), -ri)
        put_right(rt.at[h], 128, span(256, 256), rr)
        zs[span(256 * h, 256), :] = dot(pk[span(256 * h, 256), :], rt[h])
    wait3 = []
    for g in range(2):
        for h in range(2):
            for k in range(8):
                src = span(256 * h + 128 * g + SLAB * k, SLAB)
                dst = span(256 * g + 128 * h + SLAB * k, SLAB)
                zr = zs[src, 0:256]
                zi = zs[src, 256:512]
                wc = tf[0, 8 * g + k:8 * g + k + 1, :]
                ws = tf[1, 8 * g + k:8 * g + k + 1, :]
                put_left(uu, dst, 0, wc * zr - ws * zi)
                put_left(uu, dst, 256, wc * zi + ws * zr)
        out = dot(uu[span(256 * g, 256), :], wt[...])
        send3[8 * g:8 * g + 8] = jnp.where(low, out[0:128], out[128:256]).reshape(8, SLAB, 128)
        wait3.append(to_facets(2, g, send3, recv3))

    r0 = iota((FROWS, 128), 0)
    slab = jnp.zeros((FROWS, 128), jnp.int32)
    for k in range(NC):
        slab = jnp.where(((r0 >> 3) & 7) == k, col_peers[k], slab)
    rcol = s_me * FN + SLAB * slab + 8 * (r0 >> 6) + (r0 & 7)
    for g in range(2):
        fl = 1024 * (lane & 15)
        for k in range(8):
            fl = fl + jnp.where((lane >> 4) == k, rows[facet_peers[8 * g + k]], 0)
        for h in range(2):
            vc, vs = turns(rcol * (fl + 512 * h), 16, vscale)
            put_left(vb.at[g], span(128 * h, 128), 0, vc)
            put_left(vb.at[g], span(256 + 128 * h, 128), 0, vs)
    j256 = iota((M, LJ), 1)
    q32 = iota((M, LJ), 0)
    for b in range(NC):
        bc, bs = turns(j256 * (cols[col_peers[b]] + 8 * q32), 16, 1.0)
        half = bt.at[b // 4]
        r1 = 32 * (b % 4)
        put_right(half, r1, span(0, 256), bc)
        put_right(half, r1, span(256, 256), bs)
        put_right(half, 128 + r1, span(0, 256), -bs)
        put_right(half, 128 + r1, span(256, 256), bc)

    wait3[NEAR].wait_recv()
    zs[:, 0:128] = dot(vb[NEAR], right(recv3[8:16].reshape(128, 128)))
    wait3[FAR].wait_recv()
    out = zs[:, 0:128] + dot(vb[FAR], right(recv3[0:8].reshape(128, 128)))
    dd = jnp.where(low, out[0:128], out[128:256])
    ee = jnp.where(low, out[256:384], out[384:512])
    dd = dd + pltpu.roll(dd, 64, 1)
    ee = ee + pltpu.roll(ee, 64, 1)
    ee = pltpu.roll(ee, 32, 1)
    dd = dd + jnp.where(part == 0, -ee, ee)
    send4[...] = jnp.where(low, dd[0:64], dd[64:128]).reshape(NC, 8, 128)
    wait4 = [over_columns(3, g, send4, recv4) for g in range(2)]

    def columns_back(g):
        x4 = jnp.concatenate(unpack(recv4[4 * g:4 * g + 4].reshape(32, 128)), axis=0)
        y4 = pltpu.roll(x4, 32, 1)
        tiles = []
        for d in range(2):
            halves = []
            for half in range(2):
                a = []
                for k in range(4):
                    src = x4 if (k + d) % 2 == 0 else y4
                    a.append(src[32 * half + 8 * k:32 * half + 8 * k + 8])
                halves.append(
                    jnp.where(low, jnp.where(part == 0, a[0], a[1]), jnp.where(part == 0, a[2], a[3]))
                )
            tiles.append(jnp.concatenate(halves, axis=0))
        sre, sim = tiles
        for i in range(NI):
            wc = at[0, i:i + 1, span(128 * g, 128)]
            ws = at[1, i:i + 1, span(128 * g, 128)]
            put_left(ud, span(SLAB * i, SLAB), 0, sre * wc - sim * ws)
            put_left(ud, span(SLAB * i, SLAB), 128, sim * wc + sre * ws)
        return dot(ud[...], bt[g])

    wait4[NEAR].wait_recv()
    near = columns_back(NEAR)
    for i in range(NI):
        rs = span(SLAB * i, SLAB)
        for d in range(2):
            new[d, :, LJ * i:LJ * (i + 1)] = (
                sky[d, :, LJ * i:LJ * (i + 1)] + near[rs, span(256 * d, 256)]
            )
    wait4[FAR].wait_recv()
    zs[...] = columns_back(FAR)
    for i in range(NI):
        rs = span(SLAB * i, SLAB)
        ur = new[0, :, LJ * i:LJ * (i + 1)] + zs[rs, 0:256]
        ui = new[1, :, LJ * i:LJ * (i + 1)] + zs[rs, 256:512]
        mag = jnp.sqrt(ur * ur + ui * ui)
        ratio = jnp.maximum(mag - SHRINK, 0.0) / jnp.maximum(mag, SHRINK)
        new[0, :, LJ * i:LJ * (i + 1)] = ur * ratio
        new[1, :, LJ * i:LJ * (i + 1)] = ui * ratio

    wait5 = []
    columns_forward(new, send5, lambda g: wait5.append(over_columns(4, g, send5, recv5)))
    wait6 = rows_forward(vt, wait5, recv5, 5, send6, recv6)
    wait6[NEAR].wait_recv()
    for h, x in enumerate(model_half(NEAR, recv6[8:16], wz, tf, pt, zs, tt)):
        gs[span(256 * h, 256), :] = x
    wait6[FAR].wait_recv()
    parts[...] = recv6[0:8]
    for group in (wait1, wait2, wait3, wait4, wait5, wait6):
        for wait in group:
            wait.wait_send()


def local(sky_image, observed, weights, facet_offsets, subgrid_rows, subgrid_columns):
    vmem = pl.BlockSpec(memory_space=pltpu.VMEM)
    hbm = pl.BlockSpec(memory_space=pltpu.HBM)
    small = pltpu.VMEM((NC, 8, 128), F32)
    large = pltpu.VMEM((NF, SLAB, 128), F32)

    def left(rows, columns, *lead):
        return pltpu.VMEM((*lead, rows, 3 * columns), BF16)

    def right_of(rows, columns, *lead):
        return pltpu.VMEM((*lead, 3 * rows, columns), BF16)

    operands = [
        pltpu.with_memory_space_constraint(x, pltpu.HBM)
        for x in (facet_offsets.T, subgrid_rows, subgrid_columns, sky_image, observed, weights)
    ]
    halfway = pltpu.VMEM((512, 512), F32)
    parts, gs, wz, tf, pt, new = pl.pallas_call(
        kernel,
        out_shape=(
            pltpu.VMEM((8, SLAB, 128), F32),
            pltpu.VMEM((512, 512), F32),
            pltpu.VMEM((256, 512), BF16),
            pltpu.VMEM((2, NF, G), F32),
            left(512, 128, 2),
            pltpu.VMEM((2, SLAB, FN), F32),
        ),
        in_specs=[hbm] * 6,
        out_specs=(vmem,) * 6,
        scratch_shapes=[
            pltpu.SMEM((2, NF), jnp.int32),
            pltpu.SMEM((NF,), jnp.int32),
            pltpu.SMEM((NC,), jnp.int32),
            pltpu.VMEM((2, SLAB, FN), F32),
            pltpu.VMEM((2, G, G), F32),
            pltpu.VMEM((G, G), jnp.int32),
            right_of(512, 512),
            right_of(256, 512, 2),
            pltpu.VMEM((2, NI, LJ), F32),
            left(512, 128, 2),
            left(512, 128, 2),
            right_of(512, 128),
            left(512, 256),
            halfway,
            right_of(128, 512, 2),
            right_of(256, 512, 2),
            left(512, 512),
            left(512, 256),
            small, small, large, large, large, large, small, small, small, small, large, large,
            pltpu.SemaphoreType.DMA((6, 2)),
            pltpu.SemaphoreType.DMA((6, 2)),
            pltpu.SemaphoreType.DMA((6,)),
        ],
        compiler_params=pltpu.CompilerParams(
            collective_id=0, has_side_effects=True, vmem_limit_bytes=40 * 1024 * 1024
        ),
        name="imaging",
    )(*operands)
    return pl.pallas_call(
        finish_kernel,
        out_shape=(
            jax.ShapeDtypeStruct((2, SLAB, FN), F32),
            jax.ShapeDtypeStruct((2, G, G), F32),
        ),
        in_specs=[vmem] * 6,
        out_specs=(hbm, hbm),
        scratch_shapes=[
            pltpu.VMEM((2, G, G), F32),
            halfway,
            right_of(128, 512, 2),
            pltpu.SemaphoreType.DMA((5,)),
        ],
        compiler_params=pltpu.CompilerParams(vmem_limit_bytes=32 * 1024 * 1024),
        name="finish",
    )(parts, gs, wz, tf, pt, new)


def solution(mesh):
    return jax.shard_map(
        local,
        mesh=mesh,
        in_specs=(
            P(None, ("facet", "col"), None),
            P(None, "facet", "col"),
            P("facet", "col"),
            P(),
            P(),
            P(),
        ),
        out_specs=(P(None, ("facet", "col"), None), P(None, "facet", "col")),
        check_vma=False,
    )
```

```python
import math

import jax
import jax.numpy as jnp
from jax import lax
from jax.experimental import pallas as pl
from jax.experimental.pallas import tpu as pltpu
from jax.sharding import PartitionSpec as P

FN = 8192
M = 32
SLOTS = 8
NIMG = 65536
G = 256
FROWS = 128
NF = 16
NC = 8
SLAB = 16
LJ = 256
NI = 32
SHRINK = 0.5
F32 = jnp.float32
BF16 = jnp.bfloat16
MESH = pl.DeviceIdType.MESH


def iota(shape, dim):
    return lax.broadcasted_iota(jnp.int32, shape, dim)


def turns(k, bits, scale):
    n = 1 << bits
    k = k & (n - 1)
    q = (k + n // 8) >> (bits - 2)
    x = (k - (q << (bits - 2))).astype(F32) * (2.0 * math.pi / n)
    y = x * x
    s = x * (1.0 + y * (-1.0 / 6 + y * (1.0 / 120 + y * (-1.0 / 5040 + y * (1.0 / 362880)))))
    c = 1.0 + y * (-0.5 + y * (1.0 / 24 + y * (-1.0 / 720 + y * (1.0 / 40320 + y * (-1.0 / 3628800)))))
    swap = (q & 1) == 1
    cc = jnp.where(swap, s, c) * scale
    ss = jnp.where(swap, c, s) * scale
    return (
        jnp.where(((q + 1) & 2) != 0, -cc, cc),
        jnp.where((q & 2) != 0, -ss, ss),
    )


def split(x):
    high = x.astype(BF16)
    return high, (x - high.astype(F32)).astype(BF16)


def put_left(ref, rows, start, x):
    high, rest = split(x)
    k = ref.shape[-1] // 2
    n = x.shape[1]
    ref[rows, start:start + n] = high
    ref[rows, k + start:k + start + n] = rest


def put_right(ref, start, columns, x):
    high, rest = split(x)
    k = ref.shape[-2] // 3
    n = x.shape[0]
    ref[start:start + n, columns] = high
    ref[k + start:k + start + n, columns] = high
    ref[2 * k + start:2 * k + start + n, columns] = rest


def right(x):
    high, rest = split(x)
    return jnp.concatenate([high, high, rest], axis=0)


def dot(a, b):
    return lax.dot_general(a, b, (((1,), (0,)), ((), ())), preferred_element_type=F32)


def dot3(a, b):
    k = a.shape[1]
    return dot(a, b[0:k]) + dot(a[:, 0:k // 2], b[k:k + k // 2])


def span(start, size):
    return slice(start, start + size)


ALL = slice(None)
COL_STEPS = ((1, 2), (1, 1), (1, 3), (0, 2), (1, 0), (0, 1), (0, 3), (0, 0))
FACET_STEPS = (
    (2, 1, 0), (2, 1, 1), (2, 0, 0), (2, 0, 1), (1, 1, 0), (1, 1, 1), (3, 1, 0), (3, 1, 1),
    (1, 0, 0), (1, 0, 1), (3, 0, 0), (3, 0, 1), (0, 1, 0), (0, 1, 1), (0, 0, 1), (0, 0, 0),
)
COL_BACK = tuple(COL_STEPS.index((x, -z % 4)) for x, z in COL_STEPS)
FACET_CROSS = tuple(FACET_STEPS.index((y, x, 1 - k)) for y, x, k in FACET_STEPS)
FACET_CROSS_BACK = tuple(FACET_STEPS.index((-y % 4, x, 1 - k)) for y, x, k in FACET_STEPS)
FAR, NEAR = 0, 1


def lanes():
    lane = iota((1, 128), 1)
    return lane < 64, (lane >> 5) & 1


def model_half(group, parts, wz, tf, pt, zs, tt):
    low, _ = lanes()
    x = parts.reshape(128, 128)
    high = x.astype(BF16).astype(F32)
    rest = x - high
    a = jnp.concatenate(
        [
            jnp.where(low, high, pltpu.roll(rest, 64, 1)),
            jnp.where(low, pltpu.roll(high, 64, 1), rest),
        ],
        axis=0,
    ).astype(BF16)
    zs[0:256, :] = dot(jnp.concatenate([a, a], axis=1), wz[...])
    sums = []
    for h in range(2):
        for k in range(8):
            rows = span(128 * h + SLAB * k, SLAB)
            zr = zs[rows, 0:256]
            zi = zs[rows, 256:512]
            wc = tf[0, 8 * group + k:8 * group + k + 1, :]
            ws = tf[1, 8 * group + k:8 * group + k + 1, :]
            put_right(tt.at[h], SLAB * k, span(0, 256), wc * zr + ws * zi)
            put_right(tt.at[h], SLAB * k, span(256, 256), wc * zi - ws * zr)
        sums.append(dot3(pt[group, span(256 * h, 256), :], tt[h]))
    return sums


def combine(even, odd):
    (er, ei), (dr, di) = [
        (s[0:128, 0:256] + s[128:256, 256:512], s[0:128, 256:512] - s[128:256, 0:256])
        for s in (even, odd)
    ]
    return (er + dr, ei + di), (er - dr, ei - di)


def finish_kernel(parts, gs, wz, tf, pt, new, new_h, pred_h, pred, zs, tt, sem):
    store_new = pltpu.make_async_copy(new, new_h, sem.at[0])
    store_new.start()
    stores = [store_new]
    sums = model_half(FAR, parts[...], wz, tf, pt, zs, tt)
    for half, values in enumerate(combine(gs[0:256] + sums[0], gs[256:512] + sums[1])):
        for d in range(2):
            rows = span(128 * half, 128)
            pred[d, rows, :] = values[d]
            cp = pltpu.make_async_copy(pred.at[d, rows, :], pred_h.at[d, rows, :], sem.at[1 + 2 * half + d])
            cp.start()
            stores.append(cp)
    for cp in stores:
        cp.wait()


def kernel(
    offs_h, rows_h, cols_h, sky_h, obs_h, wts_h,
    parts, gs, wz, tf, pt, new,
    offs, rows, cols, sky, obs, wts,
    bm, bt, at, vt, vb, wt, pk, zs, tt, rt, uu, ud,
    send1, recv1, send2, recv2, send3, recv3, send4, recv4, send5, recv5, send6, recv6,
    ssem, rsem, isem,
):
    f = lax.axis_index("facet")
    c = lax.axis_index("col")

    loads = [
        pltpu.make_async_copy(src, dst, isem.at[n])
        for n, (src, dst) in enumerate(
            ((cols_h, cols), (offs_h, offs), (rows_h, rows), (sky_h, sky), (obs_h, obs), (wts_h, wts))
        )
    ]
    for cp in loads:
        cp.start()

    fy, fx, fk = lax.div(f, 4), lax.rem(lax.div(f, 2), 2), lax.rem(f, 2)
    cx, cz = lax.div(c, 4), lax.rem(c, 4)
    col_peers = [4 * lax.rem(cx + x, 2) + lax.rem(cz + z, 4) for x, z in COL_STEPS]
    facet_peers = [
        4 * lax.rem(fy + y, 4) + 2 * lax.rem(fx + x, 2) + lax.rem(fk + k, 2) for y, x, k in FACET_STEPS
    ]
    other = 4 * fy + 2 * fx + (1 - fk)
    barrier = pltpu.get_barrier_semaphore()
    for peer in facet_peers[:-1]:
        pl.semaphore_signal(barrier, inc=1, device_id={"facet": peer}, device_id_type=MESH)
    for peer in col_peers[:-1]:
        pl.semaphore_signal(barrier, inc=1, device_id={"facet": other, "col": peer}, device_id_type=MESH)

    def start(phase, group, send, recv, moves, own=None):
        def copy(src, dst, device):
            return pltpu.make_async_remote_copy(
                src_ref=src, dst_ref=dst, send_sem=ssem.at[phase, group], recv_sem=rsem.at[phase, group],
                device_id=device, device_id_type=MESH,
            )

        for block, slot, device in moves:
            copy(send.at[block], recv.at[slot], device).start()
        if own is not None:
            recv[own[1]] = send[own[0]]
        blocks = pl.ds(0, len(moves))
        return copy(send.at[blocks], recv.at[blocks], moves[0][2])

    def over_columns(phase, group, send, recv):
        moves = [
            (k, COL_BACK[k], {"facet": other, "col": col_peers[k]}) for k in range(4 * group, 4 * group + 4)
        ]
        return start(phase, group, send, recv, moves)

    def to_subgrids(phase, group, send, recv):
        moves = [
            (k, FACET_CROSS_BACK[k], {"facet": facet_peers[k]})
            for k in range(8 * group, 8 * group + 8)
            if k < NF - 1
        ]
        own = (NF - 1, FACET_CROSS_BACK[NF - 1]) if group == NEAR else None
        return start(phase, group, send, recv, moves, own)

    def to_facets(phase, group, send, recv):
        moves, own = [], None
        for k in range(8 * group, 8 * group + 8):
            if FACET_CROSS[k] < NF - 1:
                moves.append((k, FACET_CROSS_BACK[k], {"facet": facet_peers[FACET_CROSS[k]]}))
            else:
                own = (k, FACET_CROSS_BACK[k])
        return start(phase, group, send, recv, moves, own)

    low, part = lanes()
    lane = iota((1, 128), 1)

    def unpack(x):
        y = pltpu.roll(x, 64, 1)
        return jnp.where(low, x, y), jnp.where(low, y, x)

    l256 = iota((1, LJ), 1)
    cv = 8 * (l256 & 31)
    loads[0].wait()
    for b in range(NC):
        cv = cv + jnp.where((l256 >> 5) == b, cols[col_peers[b]], 0)
    steps = iota((SLAB, LJ), 0)
    c1, s1 = turns((SLAB * steps) * cv, 16, 1.0)
    c0, s0 = turns(steps * cv, 16, 1.0)
    for k in range(SLAB):
        bc = c1[k:k + 1] * c0 - s1[k:k + 1] * s0
        bs = s1[k:k + 1] * c0 + c1[k:k + 1] * s0
        put_right(bm, SLAB * k, span(0, 256), bc)
        put_right(bm, SLAB * k, span(256, 256), -bs)
        put_right(bm, 256 + SLAB * k, span(0, 256), bs)
        put_right(bm, 256 + SLAB * k, span(256, 256), bc)
    loads[1].wait()
    s_me = offs[0, other]
    t_me = offs[1, f]
    ac, as_ = turns((t_me * FN + LJ * iota((NI, LJ), 0)) * cv, 16, 1.0 / math.sqrt(FN))
    at[0] = ac
    at[1] = as_

    def columns_forward(image, send, launch):
        for i in range(NI):
            for d in range(2):
                put_left(uu, span(SLAB * i, SLAB), 256 * d, image[d, :, LJ * i:LJ * (i + 1)])
        zs[...] = dot3(uu[...], bm[...])
        re = jnp.zeros((SLAB, LJ), F32)
        im = jnp.zeros((SLAB, LJ), F32)
        for i in range(NI):
            zr = zs[span(SLAB * i, SLAB), 0:256]
            zi = zs[span(SLAB * i, SLAB), 256:512]
            wc = at[0, i:i + 1, :]
            ws = at[1, i:i + 1, :]
            re = re + (wc * zr + ws * zi)
            im = im + (wc * zi - ws * zr)
        for g in range(2):
            rot_re = [re[:, span(128 * g, 128)]]
            rot_im = [im[:, span(128 * g, 128)]]
            for m in range(1, 4):
                rot_re.append(pltpu.roll(rot_re[0], 32 * m, 1))
                rot_im.append(pltpu.roll(rot_im[0], 32 * m, 1))
            for k in range(4):
                send[4 * g + k] = jnp.where(
                    low,
                    jnp.where(part == 0, rot_re[(4 - k) % 4][0:8], rot_im[(5 - k) % 4][0:8]),
                    jnp.where(part == 0, rot_re[(6 - k) % 4][8:16], rot_im[(7 - k) % 4][8:16]),
                )
            launch(g)

    def row_operand(group, recv):
        x = jnp.concatenate(unpack(recv[4 * group:4 * group + 4].reshape(32, 128)), axis=0)
        y = pltpu.roll(x, 32, 1)
        y = jnp.where(part == 0, y, -y)
        return right(jnp.concatenate([x, y], axis=0))

    def rows_forward(waits, recv, phase, send, into):
        waits[NEAR].wait_recv()
        zs[:, 0:128] = dot3(vt[NEAR], row_operand(NEAR, recv))
        waits[FAR].wait_recv()
        operand = row_operand(FAR, recv)
        later = []
        for g in range(2):
            out = zs[span(256 * g, 256), 0:128] + dot3(vt[FAR, span(256 * g, 256), :], operand)
            send[8 * g:8 * g + 8] = jnp.where(low, out[0:128], out[128:256]).reshape(8, SLAB, 128)
            later.append(to_subgrids(phase, g, send, into))
        return later

    loads[3].wait()
    wait1 = []

    def launch1(g):
        if g == FAR:
            pl.semaphore_wait(barrier, NF - 1 + NC - 1)
        wait1.append(over_columns(0, g, send1, recv1))

    columns_forward(sky, send1, launch1)

    loads[2].wait()

    p16 = iota((SLAB, 128), 0)
    l128 = iota((SLAB, 128), 1)
    vscale = 1.0 / math.sqrt(FROWS)
    lane1 = lane & 63
    for g in range(2):
        slab = jnp.zeros((1, 128), jnp.int32)
        for k in range(4):
            slab = jnp.where(((lane1 >> 3) & 3) == k, col_peers[4 * g + k], slab)
        rlane = s_me * FN + SLAB * slab + 8 * (lane1 >> 5) + (lane1 & 7)
        for a in range(NF):
            for h in range(2):
                vc, vs = turns(rlane * (rows[facet_peers[a]] + 512 * (2 * p16 + h)), 16, vscale)
                r0 = 256 * (a // 8) + 128 * h + SLAB * (a % 8)
                put_left(vt.at[g], span(r0, SLAB), 0, jnp.where(low, vc, vs))
    wait2 = rows_forward(wait1, recv1, 1, send2, recv2)

    for d in range(0, M, SLAB):
        wc, ws = turns((d + iota((SLAB, G), 0)) * iota((SLAB, G), 1), 8, 1.0 / 16)
        for r0, n, x in ((d, 0, wc), (d, 256, -ws), (M + d, 0, ws), (M + d, 256, wc)):
            high, rest = split(x)
            wz[r0:r0 + SLAB, n:n + 256] = high
            wz[64 + r0:64 + r0 + SLAB, n:n + 256] = high
            wz[128 + r0:128 + r0 + SLAB, n:n + 256] = rest
    wz[192:256, :] = jnp.zeros((64, 512), BF16)
    tv = jnp.zeros((NF, G), jnp.int32)
    i16 = iota((NF, G), 0)
    for a in range(NF):
        tv = jnp.where(i16 == a, offs[1, facet_peers[a]], tv)
    tc, ts = turns(tv * iota((NF, G), 1), 3, 1.0)
    tf[0] = tc
    tf[1] = ts
    for g in range(2):
        place = 2 * (lane & 15)
        for k in range(8):
            place = place + jnp.where((lane >> 4) == k, offs[0, facet_peers[8 * g + k]] * M, 0)
        for h in range(2):
            pc, ps_ = turns(iota((128, 128), 0) * (place + h), 8, 1.0 / 16)
            put_left(pt.at[g], span(256 * h, 128), 0, pc)
            put_left(pt.at[g], span(256 * h + 128, 128), 0, ps_)
    for h in range(2):
        for a in range(NF):
            kc, ks = turns((offs[0, facet_peers[a]] * M + h + 2 * p16) * l128, 8, 1.0 / 16)
            put_left(pk, span(256 * h + SLAB * a, SLAB), 0, kc)
            put_left(pk, span(256 * h + SLAB * a, SLAB), 128, ks)
    wc_, ws_ = turns(iota((G, 128), 0) * (lane & 31), 8, 1.0 / 16)
    put_right(wt, 0, ALL, jnp.where(part == 0, wc_, ws_))
    put_right(wt, 256, ALL, jnp.where(part == 0, -ws_, wc_))
    wait2[NEAR].wait_recv()
    for h, x in enumerate(model_half(NEAR, recv2[8:16], wz, tf, pt, zs, tt)):
        gs[span(256 * h, 256), :] = x
    loads[4].wait()
    loads[5].wait()
    wait2[FAR].wait_recv()

    sums = model_half(FAR, recv2[0:8], wz, tf, pt, zs, tt)
    resid = []
    for half, (mr, mi) in enumerate(combine(gs[0:256] + sums[0], gs[256:512] + sums[1])):
        rs = span(128 * half, 128)
        mask = wts[rs, :].astype(F32)
        resid.append((mask * (obs[0, rs, :] - mr), mask * (obs[1, rs, :] - mi)))
    for h in range(2):
        rr, ri = [
            resid[0][d] + resid[1][d] if h == 0 else resid[0][d] - resid[1][d] for d in range(2)
        ]
        put_right(rt.at[h], 0, span(0, 256), rr)
        put_right(rt.at[h], 0, span(256, 256), ri)
        put_right(rt.at[h], 128, span(0, 256), -ri)
        put_right(rt.at[h], 128, span(256, 256), rr)
        zs[span(256 * h, 256), :] = dot3(pk[span(256 * h, 256), :], rt[h])
    wait3 = []
    for g in range(2):
        for h in range(2):
            for k in range(8):
                src = span(256 * h + 128 * g + SLAB * k, SLAB)
                dst = span(256 * g + 128 * h + SLAB * k, SLAB)
                zr = zs[src, 0:256]
                zi = zs[src, 256:512]
                wc = tf[0, 8 * g + k:8 * g + k + 1, :]
                ws = tf[1, 8 * g + k:8 * g + k + 1, :]
                put_left(uu, dst, 0, wc * zr - ws * zi)
                put_left(uu, dst, 256, wc * zi + ws * zr)
        out = dot3(uu[span(256 * g, 256), :], wt[...])
        send3[8 * g:8 * g + 8] = jnp.where(low, out[0:128], out[128:256]).reshape(8, SLAB, 128)
        wait3.append(to_facets(2, g, send3, recv3))

    r0 = iota((FROWS, 128), 0)
    slab = jnp.zeros((FROWS, 128), jnp.int32)
    for k in range(NC):
        slab = jnp.where(((r0 >> 3) & 7) == k, col_peers[k], slab)
    rcol = s_me * FN + SLAB * slab + 8 * (r0 >> 6) + (r0 & 7)
    for g in range(2):
        fl = 1024 * (lane & 15)
        for k in range(8):
            fl = fl + jnp.where((lane >> 4) == k, rows[facet_peers[8 * g + k]], 0)
        for h in range(2):
            vc, vs = turns(rcol * (fl + 512 * h), 16, vscale)
            put_left(vb.at[g], span(128 * h, 128), 0, vc)
            put_left(vb.at[g], span(256 + 128 * h, 128), 0, vs)
    j256 = iota((M, LJ), 1)
    q32 = iota((M, LJ), 0)
    for b in range(NC):
        bc, bs = turns(j256 * (cols[col_peers[b]] + 8 * q32), 16, 1.0)
        half = bt.at[b // 4]
        r1 = 32 * (b % 4)
        put_right(half, r1, span(0, 256), bc)
        put_right(half, r1, span(256, 256), bs)
        put_right(half, 128 + r1, span(0, 256), -bs)
        put_right(half, 128 + r1, span(256, 256), bc)

    wait3[NEAR].wait_recv()
    zs[:, 0:128] = dot3(vb[NEAR], right(recv3[8:16].reshape(128, 128)))
    wait3[FAR].wait_recv()
    out = zs[:, 0:128] + dot3(vb[FAR], right(recv3[0:8].reshape(128, 128)))
    dd = jnp.where(low, out[0:128], out[128:256])
    ee = jnp.where(low, out[256:384], out[384:512])
    dd = dd + pltpu.roll(dd, 64, 1)
    ee = ee + pltpu.roll(ee, 64, 1)
    ee = pltpu.roll(ee, 32, 1)
    dd = dd + jnp.where(part == 0, -ee, ee)
    send4[...] = jnp.where(low, dd[0:64], dd[64:128]).reshape(NC, 8, 128)
    wait4 = [over_columns(3, g, send4, recv4) for g in range(2)]

    def columns_back(g):
        x4 = jnp.concatenate(unpack(recv4[4 * g:4 * g + 4].reshape(32, 128)), axis=0)
        y4 = pltpu.roll(x4, 32, 1)
        tiles = []
        for d in range(2):
            halves = []
            for half in range(2):
                a = []
                for k in range(4):
                    src = x4 if (k + d) % 2 == 0 else y4
                    a.append(src[32 * half + 8 * k:32 * half + 8 * k + 8])
                halves.append(
                    jnp.where(low, jnp.where(part == 0, a[0], a[1]), jnp.where(part == 0, a[2], a[3]))
                )
            tiles.append(jnp.concatenate(halves, axis=0))
        sre, sim = tiles
        for i in range(NI):
            wc = at[0, i:i + 1, span(128 * g, 128)]
            ws = at[1, i:i + 1, span(128 * g, 128)]
            put_left(ud, span(SLAB * i, SLAB), 0, sre * wc - sim * ws)
            put_left(ud, span(SLAB * i, SLAB), 128, sim * wc + sre * ws)
        return dot3(ud[...], bt[g])

    wait4[NEAR].wait_recv()
    near = columns_back(NEAR)
    for i in range(NI):
        rs = span(SLAB * i, SLAB)
        for d in range(2):
            new[d, :, LJ * i:LJ * (i + 1)] = (
                sky[d, :, LJ * i:LJ * (i + 1)] + near[rs, span(256 * d, 256)]
            )
    wait4[FAR].wait_recv()
    zs[...] = columns_back(FAR)
    for i in range(NI):
        rs = span(SLAB * i, SLAB)
        ur = new[0, :, LJ * i:LJ * (i + 1)] + zs[rs, 0:256]
        ui = new[1, :, LJ * i:LJ * (i + 1)] + zs[rs, 256:512]
        mag = jnp.sqrt(ur * ur + ui * ui)
        ratio = jnp.maximum(mag - SHRINK, 0.0) / jnp.maximum(mag, SHRINK)
        new[0, :, LJ * i:LJ * (i + 1)] = ur * ratio
        new[1, :, LJ * i:LJ * (i + 1)] = ui * ratio

    wait5 = []
    columns_forward(new, send5, lambda g: wait5.append(over_columns(4, g, send5, recv5)))
    wait6 = rows_forward(wait5, recv5, 5, send6, recv6)
    wait6[NEAR].wait_recv()
    for h, x in enumerate(model_half(NEAR, recv6[8:16], wz, tf, pt, zs, tt)):
        gs[span(256 * h, 256), :] = x
    wait6[FAR].wait_recv()
    parts[...] = recv6[0:8]
    for group in (wait1, wait2, wait3, wait4, wait5, wait6):
        for wait in group:
            wait.wait_send()


def local(sky_image, observed, weights, facet_offsets, subgrid_rows, subgrid_columns):
    vmem = pl.BlockSpec(memory_space=pltpu.VMEM)
    hbm = pl.BlockSpec(memory_space=pltpu.HBM)
    small = pltpu.VMEM((NC, 8, 128), F32)
    large = pltpu.VMEM((NF, SLAB, 128), F32)

    def left(rows, columns, *lead):
        return pltpu.VMEM((*lead, rows, 2 * columns), BF16)

    def right_of(rows, columns, *lead):
        return pltpu.VMEM((*lead, 3 * rows, columns), BF16)

    operands = [
        pltpu.with_memory_space_constraint(x, pltpu.HBM)
        for x in (facet_offsets.T, subgrid_rows, subgrid_columns, sky_image, observed, weights)
    ]
    halfway = pltpu.VMEM((512, 512), F32)
    parts, gs, wz, tf, pt, new = pl.pallas_call(
        kernel,
        out_shape=(
            pltpu.VMEM((8, SLAB, 128), F32),
            pltpu.VMEM((512, 512), F32),
            pltpu.VMEM((256, 512), BF16),
            pltpu.VMEM((2, NF, G), F32),
            left(512, 128, 2),
            pltpu.VMEM((2, SLAB, FN), F32),
        ),
        in_specs=[hbm] * 6,
        out_specs=(vmem,) * 6,
        scratch_shapes=[
            pltpu.SMEM((2, NF), jnp.int32),
            pltpu.SMEM((NF,), jnp.int32),
            pltpu.SMEM((NC,), jnp.int32),
            pltpu.VMEM((2, SLAB, FN), F32),
            pltpu.VMEM((2, G, G), F32),
            pltpu.VMEM((G, G), jnp.int32),
            right_of(512, 512),
            right_of(256, 512, 2),
            pltpu.VMEM((2, NI, LJ), F32),
            left(512, 128, 2),
            left(512, 128, 2),
            right_of(512, 128),
            left(512, 256),
            halfway,
            right_of(128, 512, 2),
            right_of(256, 512, 2),
            left(512, 512),
            left(512, 256),
            small, small, large, large, large, large, small, small, small, small, large, large,
            pltpu.SemaphoreType.DMA((6, 2)),
            pltpu.SemaphoreType.DMA((6, 2)),
            pltpu.SemaphoreType.DMA((6,)),
        ],
        compiler_params=pltpu.CompilerParams(
            collective_id=0, has_side_effects=True, vmem_limit_bytes=40 * 1024 * 1024
        ),
        name="imaging",
    )(*operands)
    return pl.pallas_call(
        finish_kernel,
        out_shape=(
            jax.ShapeDtypeStruct((2, SLAB, FN), F32),
            jax.ShapeDtypeStruct((2, G, G), F32),
        ),
        in_specs=[vmem] * 6,
        out_specs=(hbm, hbm),
        scratch_shapes=[
            pltpu.VMEM((2, G, G), F32),
            halfway,
            right_of(128, 512, 2),
            pltpu.SemaphoreType.DMA((5,)),
        ],
        compiler_params=pltpu.CompilerParams(vmem_limit_bytes=32 * 1024 * 1024),
        name="finish",
    )(parts, gs, wz, tf, pt, new)


def solution(mesh):
    return jax.shard_map(
        local,
        mesh=mesh,
        in_specs=(
            P(None, ("facet", "col"), None),
            P(None, "facet", "col"),
            P("facet", "col"),
            P(),
            P(),
            P(),
        ),
        out_specs=(P(None, ("facet", "col"), None), P(None, "facet", "col")),
        check_vma=False,
    )
```

```python
import math

import jax
import jax.numpy as jnp
from jax import lax
from jax.experimental import pallas as pl
from jax.experimental.pallas import tpu as pltpu
from jax.sharding import PartitionSpec as P

FN = 8192
M = 32
SLOTS = 8
NIMG = 65536
G = 256
FROWS = 128
NF = 16
NC = 8
SLAB = 16
LJ = 256
NI = 32
SHRINK = 0.5
F32 = jnp.float32
BF16 = jnp.bfloat16
MESH = pl.DeviceIdType.MESH


def iota(shape, dim):
    return lax.broadcasted_iota(jnp.int32, shape, dim)


def turns(k, bits, scale):
    n = 1 << bits
    k = k & (n - 1)
    q = (k + n // 8) >> (bits - 2)
    x = (k - (q << (bits - 2))).astype(F32) * (2.0 * math.pi / n)
    y = x * x
    s = x * (1.0 + y * (-1.0 / 6 + y * (1.0 / 120 + y * (-1.0 / 5040 + y * (1.0 / 362880)))))
    c = 1.0 + y * (-0.5 + y * (1.0 / 24 + y * (-1.0 / 720 + y * (1.0 / 40320 + y * (-1.0 / 3628800)))))
    swap = (q & 1) == 1
    cc = jnp.where(swap, s, c) * scale
    ss = jnp.where(swap, c, s) * scale
    return (
        jnp.where(((q + 1) & 2) != 0, -cc, cc),
        jnp.where((q & 2) != 0, -ss, ss),
    )


def split(x):
    high = x.astype(BF16)
    return high, (x - high.astype(F32)).astype(BF16)


def put_left(ref, rows, start, x):
    high, rest = split(x)
    k = ref.shape[-1] // 2
    n = x.shape[1]
    ref[rows, start:start + n] = high
    ref[rows, k + start:k + start + n] = rest


def put_right(ref, start, columns, x):
    high, rest = split(x)
    k = ref.shape[-2] // 3
    n = x.shape[0]
    ref[start:start + n, columns] = high
    ref[k + start:k + start + n, columns] = high
    ref[2 * k + start:2 * k + start + n, columns] = rest


def right(x):
    high, rest = split(x)
    return jnp.concatenate([high, high, rest], axis=0)


def dot(a, b):
    return lax.dot_general(a, b, (((1,), (0,)), ((), ())), preferred_element_type=F32)


def dot3(a, b):
    k = a.shape[1]
    return dot(a, b[0:k]) + dot(a[:, 0:k // 2], b[k:k + k // 2])


def span(start, size):
    return slice(start, start + size)


ALL = slice(None)
COL_STEPS = ((1, 2), (1, 1), (1, 3), (0, 2), (1, 0), (0, 1), (0, 3), (0, 0))
FACET_STEPS = (
    (2, 1, 0), (2, 1, 1), (2, 0, 0), (2, 0, 1), (1, 1, 0), (1, 1, 1), (3, 1, 0), (3, 1, 1),
    (1, 0, 0), (1, 0, 1), (3, 0, 0), (3, 0, 1), (0, 1, 0), (0, 1, 1), (0, 0, 1), (0, 0, 0),
)
COL_BACK = tuple(COL_STEPS.index((x, -z % 4)) for x, z in COL_STEPS)
FACET_CROSS = tuple(FACET_STEPS.index((y, x, 1 - k)) for y, x, k in FACET_STEPS)
FACET_CROSS_BACK = tuple(FACET_STEPS.index((-y % 4, x, 1 - k)) for y, x, k in FACET_STEPS)
FAR, NEAR = 0, 1


def lanes():
    lane = iota((1, 128), 1)
    return lane < 64, (lane >> 5) & 1


def model_half(group, parts, wz, tf, pt, zs, tt):
    low, _ = lanes()
    x = parts.reshape(128, 128)
    high = x.astype(BF16).astype(F32)
    rest = x - high
    a = jnp.concatenate(
        [
            jnp.where(low, high, pltpu.roll(rest, 64, 1)),
            jnp.where(low, pltpu.roll(high, 64, 1), rest),
        ],
        axis=0,
    ).astype(BF16)
    zs[0:256, :] = dot(jnp.concatenate([a, a], axis=1), wz[...])
    sums = []
    for h in range(2):
        for k in range(8):
            rows = span(128 * h + SLAB * k, SLAB)
            zr = zs[rows, 0:256]
            zi = zs[rows, 256:512]
            wc = tf[0, 8 * group + k:8 * group + k + 1, :]
            ws = tf[1, 8 * group + k:8 * group + k + 1, :]
            put_right(tt.at[h], SLAB * k, span(0, 256), wc * zr + ws * zi)
            put_right(tt.at[h], SLAB * k, span(256, 256), wc * zi - ws * zr)
        sums.append(dot3(pt[group, span(256 * h, 256), :], tt[h]))
    return sums


def combine(even, odd):
    (er, ei), (dr, di) = [
        (s[0:128, 0:256] + s[128:256, 256:512], s[0:128, 256:512] - s[128:256, 0:256])
        for s in (even, odd)
    ]
    return (er + dr, ei + di), (er - dr, ei - di)


def finish_kernel(parts, gs, wz, tf, pt, new, new_h, pred_h, pred, zs, tt, sem):
    store_new = pltpu.make_async_copy(new, new_h, sem.at[0])
    store_new.start()
    stores = [store_new]
    sums = model_half(FAR, parts[...], wz, tf, pt, zs, tt)
    for half, values in enumerate(combine(gs[0:256] + sums[0], gs[256:512] + sums[1])):
        for d in range(2):
            rows = span(128 * half, 128)
            pred[d, rows, :] = values[d]
            cp = pltpu.make_async_copy(pred.at[d, rows, :], pred_h.at[d, rows, :], sem.at[1 + 2 * half + d])
            cp.start()
            stores.append(cp)
    for cp in stores:
        cp.wait()


def kernel(
    offs_h, rows_h, cols_h, sky_h, obs_h, wts_h,
    parts, gs, wz, tf, pt, new,
    offs, rows, cols, sky, obs, wts,
    bm, bt, at, vt, vb, wt, pk, zs, tt, rt, uu, ud,
    send1, recv1, send2, recv2, send3, recv3, send4, recv4, send5, recv5, send6, recv6,
    ssem, rsem, isem,
):
    f = lax.axis_index("facet")
    c = lax.axis_index("col")

    loads = [
        pltpu.make_async_copy(src, dst, isem.at[n])
        for n, (src, dst) in enumerate(
            ((sky_h, sky), (cols_h, cols), (offs_h, offs), (rows_h, rows), (obs_h, obs), (wts_h, wts))
        )
    ]
    for cp in loads:
        cp.start()

    fy, fx, fk = lax.div(f, 4), lax.rem(lax.div(f, 2), 2), lax.rem(f, 2)
    cx, cz = lax.div(c, 4), lax.rem(c, 4)
    col_peers = [4 * lax.rem(cx + x, 2) + lax.rem(cz + z, 4) for x, z in COL_STEPS]
    facet_peers = [
        4 * lax.rem(fy + y, 4) + 2 * lax.rem(fx + x, 2) + lax.rem(fk + k, 2) for y, x, k in FACET_STEPS
    ]
    other = 4 * fy + 2 * fx + (1 - fk)
    barrier = pltpu.get_barrier_semaphore()
    for peer in facet_peers[:-1]:
        pl.semaphore_signal(barrier, inc=1, device_id={"facet": peer}, device_id_type=MESH)
    for peer in col_peers[:-1]:
        pl.semaphore_signal(barrier, inc=1, device_id={"facet": other, "col": peer}, device_id_type=MESH)

    def start(phase, group, send, recv, moves, own=None):
        def copy(src, dst, device):
            return pltpu.make_async_remote_copy(
                src_ref=src, dst_ref=dst, send_sem=ssem.at[phase, group], recv_sem=rsem.at[phase, group],
                device_id=device, device_id_type=MESH,
            )

        for block, slot, device in moves:
            copy(send.at[block], recv.at[slot], device).start()
        if own is not None:
            recv[own[1]] = send[own[0]]
        blocks = pl.ds(0, len(moves))
        return copy(send.at[blocks], recv.at[blocks], moves[0][2])

    def over_columns(phase, group, send, recv):
        moves = [
            (k, COL_BACK[k], {"facet": other, "col": col_peers[k]}) for k in range(4 * group, 4 * group + 4)
        ]
        return start(phase, group, send, recv, moves)

    def to_subgrids(phase, group, send, recv):
        moves = [
            (k, FACET_CROSS_BACK[k], {"facet": facet_peers[k]})
            for k in range(8 * group, 8 * group + 8)
            if k < NF - 1
        ]
        own = (NF - 1, FACET_CROSS_BACK[NF - 1]) if group == NEAR else None
        return start(phase, group, send, recv, moves, own)

    def to_facets(phase, group, send, recv):
        moves, own = [], None
        for k in range(8 * group, 8 * group + 8):
            if FACET_CROSS[k] < NF - 1:
                moves.append((k, FACET_CROSS_BACK[k], {"facet": facet_peers[FACET_CROSS[k]]}))
            else:
                own = (k, FACET_CROSS_BACK[k])
        return start(phase, group, send, recv, moves, own)

    low, part = lanes()
    lane = iota((1, 128), 1)

    def unpack(x):
        y = pltpu.roll(x, 64, 1)
        return jnp.where(low, x, y), jnp.where(low, y, x)

    l256 = iota((1, LJ), 1)
    cv = 8 * (l256 & 31)
    loads[1].wait()
    for b in range(NC):
        cv = cv + jnp.where((l256 >> 5) == b, cols[col_peers[b]], 0)
    steps = iota((SLAB, LJ), 0)
    c1, s1 = turns((SLAB * steps) * cv, 16, 1.0)
    c0, s0 = turns(steps * cv, 16, 1.0)
    for k in range(SLAB):
        bc = c1[k:k + 1] * c0 - s1[k:k + 1] * s0
        bs = s1[k:k + 1] * c0 + c1[k:k + 1] * s0
        put_right(bm, SLAB * k, span(0, 256), bc)
        put_right(bm, SLAB * k, span(256, 256), -bs)
        put_right(bm, 256 + SLAB * k, span(0, 256), bs)
        put_right(bm, 256 + SLAB * k, span(256, 256), bc)
    loads[2].wait()
    s_me = offs[0, other]
    t_me = offs[1, f]
    ac, as_ = turns((t_me * FN + LJ * iota((NI, LJ), 0)) * cv, 16, 1.0 / math.sqrt(FN))
    at[0] = ac
    at[1] = as_

    def columns_forward(send, launch):
        zs[...] = dot3(uu[...], bm[...])
        re = jnp.zeros((SLAB, LJ), F32)
        im = jnp.zeros((SLAB, LJ), F32)
        for i in range(NI):
            zr = zs[span(SLAB * i, SLAB), 0:256]
            zi = zs[span(SLAB * i, SLAB), 256:512]
            wc = at[0, i:i + 1, :]
            ws = at[1, i:i + 1, :]
            re = re + (wc * zr + ws * zi)
            im = im + (wc * zi - ws * zr)
        for g in range(2):
            rot_re = [re[:, span(128 * g, 128)]]
            rot_im = [im[:, span(128 * g, 128)]]
            for m in range(1, 4):
                rot_re.append(pltpu.roll(rot_re[0], 32 * m, 1))
                rot_im.append(pltpu.roll(rot_im[0], 32 * m, 1))
            for k in range(4):
                send[4 * g + k] = jnp.where(
                    low,
                    jnp.where(part == 0, rot_re[(4 - k) % 4][0:8], rot_im[(5 - k) % 4][0:8]),
                    jnp.where(part == 0, rot_re[(6 - k) % 4][8:16], rot_im[(7 - k) % 4][8:16]),
                )
            launch(g)

    def row_operand(group, recv):
        x = jnp.concatenate(unpack(recv[4 * group:4 * group + 4].reshape(32, 128)), axis=0)
        y = pltpu.roll(x, 32, 1)
        y = jnp.where(part == 0, y, -y)
        return right(jnp.concatenate([x, y], axis=0))

    def rows_forward(waits, recv, phase, send, into):
        waits[NEAR].wait_recv()
        zs[:, 0:128] = dot3(vt[NEAR], row_operand(NEAR, recv))
        waits[FAR].wait_recv()
        operand = row_operand(FAR, recv)
        later = []
        for g in range(2):
            out = zs[span(256 * g, 256), 0:128] + dot3(vt[FAR, span(256 * g, 256), :], operand)
            send[8 * g:8 * g + 8] = jnp.where(low, out[0:128], out[128:256]).reshape(8, SLAB, 128)
            later.append(to_subgrids(phase, g, send, into))
        return later

    loads[0].wait()
    wait1 = []

    def launch1(g):
        if g == FAR:
            pl.semaphore_wait(barrier, NF - 1 + NC - 1)
        wait1.append(over_columns(0, g, send1, recv1))

    for i in range(NI):
        for d in range(2):
            put_left(uu, span(SLAB * i, SLAB), 256 * d, sky[d, :, LJ * i:LJ * (i + 1)])
    columns_forward(send1, launch1)

    loads[3].wait()

    p16 = iota((SLAB, 128), 0)
    l128 = iota((SLAB, 128), 1)
    vscale = 1.0 / math.sqrt(FROWS)
    lane1 = lane & 63
    for g in range(2):
        slab = jnp.zeros((1, 128), jnp.int32)
        for k in range(4):
            slab = jnp.where(((lane1 >> 3) & 3) == k, col_peers[4 * g + k], slab)
        rlane = s_me * FN + SLAB * slab + 8 * (lane1 >> 5) + (lane1 & 7)
        for a in range(NF):
            for h in range(2):
                vc, vs = turns(rlane * (rows[facet_peers[a]] + 512 * (2 * p16 + h)), 16, vscale)
                r0 = 256 * (a // 8) + 128 * h + SLAB * (a % 8)
                put_left(vt.at[g], span(r0, SLAB), 0, jnp.where(low, vc, vs))
    wait2 = rows_forward(wait1, recv1, 1, send2, recv2)

    for d in range(0, M, SLAB):
        wc, ws = turns((d + iota((SLAB, G), 0)) * iota((SLAB, G), 1), 8, 1.0 / 16)
        for r0, n, x in ((d, 0, wc), (d, 256, -ws), (M + d, 0, ws), (M + d, 256, wc)):
            high, rest = split(x)
            wz[r0:r0 + SLAB, n:n + 256] = high
            wz[64 + r0:64 + r0 + SLAB, n:n + 256] = high
            wz[128 + r0:128 + r0 + SLAB, n:n + 256] = rest
    wz[192:256, :] = jnp.zeros((64, 512), BF16)
    tv = jnp.zeros((NF, G), jnp.int32)
    i16 = iota((NF, G), 0)
    for a in range(NF):
        tv = jnp.where(i16 == a, offs[1, facet_peers[a]], tv)
    tc, ts = turns(tv * iota((NF, G), 1), 3, 1.0)
    tf[0] = tc
    tf[1] = ts
    for g in range(2):
        place = 2 * (lane & 15)
        for k in range(8):
            place = place + jnp.where((lane >> 4) == k, offs[0, facet_peers[8 * g + k]] * M, 0)
        for h in range(2):
            pc, ps_ = turns(iota((128, 128), 0) * (place + h), 8, 1.0 / 16)
            put_left(pt.at[g], span(256 * h, 128), 0, pc)
            put_left(pt.at[g], span(256 * h + 128, 128), 0, ps_)
    for h in range(2):
        for a in range(NF):
            kc, ks = turns((offs[0, facet_peers[a]] * M + h + 2 * p16) * l128, 8, 1.0 / 16)
            put_left(pk, span(256 * h + SLAB * a, SLAB), 0, kc)
            put_left(pk, span(256 * h + SLAB * a, SLAB), 128, ks)
    wc_, ws_ = turns(iota((G, 128), 0) * (lane & 31), 8, 1.0 / 16)
    put_right(wt, 0, ALL, jnp.where(part == 0, wc_, ws_))
    put_right(wt, 256, ALL, jnp.where(part == 0, -ws_, wc_))
    wait2[NEAR].wait_recv()
    for h, x in enumerate(model_half(NEAR, recv2[8:16], wz, tf, pt, zs, tt)):
        gs[span(256 * h, 256), :] = x
    loads[4].wait()
    loads[5].wait()
    wait2[FAR].wait_recv()

    sums = model_half(FAR, recv2[0:8], wz, tf, pt, zs, tt)
    resid = []
    for half, (mr, mi) in enumerate(combine(gs[0:256] + sums[0], gs[256:512] + sums[1])):
        rs = span(128 * half, 128)
        mask = wts[rs, :].astype(F32)
        resid.append((mask * (obs[0, rs, :] - mr), mask * (obs[1, rs, :] - mi)))
    for h in range(2):
        rr, ri = [
            resid[0][d] + resid[1][d] if h == 0 else resid[0][d] - resid[1][d] for d in range(2)
        ]
        put_right(rt.at[h], 0, span(0, 256), rr)
        put_right(rt.at[h], 0, span(256, 256), ri)
        put_right(rt.at[h], 128, span(0, 256), -ri)
        put_right(rt.at[h], 128, span(256, 256), rr)
        zs[span(256 * h, 256), :] = dot3(pk[span(256 * h, 256), :], rt[h])
    wait3 = []
    for g in range(2):
        for h in range(2):
            for k in range(8):
                src = span(256 * h + 128 * g + SLAB * k, SLAB)
                dst = span(256 * g + 128 * h + SLAB * k, SLAB)
                zr = zs[src, 0:256]
                zi = zs[src, 256:512]
                wc = tf[0, 8 * g + k:8 * g + k + 1, :]
                ws = tf[1, 8 * g + k:8 * g + k + 1, :]
                put_left(uu, dst, 0, wc * zr - ws * zi)
                put_left(uu, dst, 256, wc * zi + ws * zr)
        out = dot3(uu[span(256 * g, 256), :], wt[...])
        send3[8 * g:8 * g + 8] = jnp.where(low, out[0:128], out[128:256]).reshape(8, SLAB, 128)
        wait3.append(to_facets(2, g, send3, recv3))

    r0 = iota((64, 128), 0)
    for t in range(2):
        slab = jnp.zeros((64, 128), jnp.int32)
        for k in range(4):
            slab = jnp.where(((r0 >> 3) & 3) == k, col_peers[4 * t + k], slab)
        rcol = s_me * FN + SLAB * slab + 8 * (r0 >> 5) + (r0 & 7)
        for g in range(2):
            fl = 1024 * (lane & 15)
            for k in range(8):
                fl = fl + jnp.where((lane >> 4) == k, rows[facet_peers[8 * g + k]], 0)
            for h in range(2):
                vc, vs = turns(rcol * (fl + 512 * h), 16, vscale)
                put_left(vb.at[g], span(256 * t + 64 * h, 64), 0, vc)
                put_left(vb.at[g], span(256 * t + 128 + 64 * h, 64), 0, vs)
    j256 = iota((M, LJ), 1)
    q32 = iota((M, LJ), 0)
    for b in range(NC):
        bc, bs = turns(j256 * (cols[col_peers[b]] + 8 * q32), 16, 1.0)
        half = bt.at[b // 4]
        r1 = 32 * (b % 4)
        put_right(half, r1, span(0, 256), bc)
        put_right(half, r1, span(256, 256), bs)
        put_right(half, 128 + r1, span(0, 256), -bs)
        put_right(half, 128 + r1, span(256, 256), bc)

    wait3[NEAR].wait_recv()
    zs[:, 0:128] = dot3(vb[NEAR], right(recv3[8:16].reshape(128, 128)))
    wait3[FAR].wait_recv()
    operand = right(recv3[0:8].reshape(128, 128))
    wait4 = []
    for t in range(2):
        out = zs[span(256 * t, 256), 0:128] + dot3(vb[FAR, span(256 * t, 256), :], operand)
        dd = jnp.where(low, out[0:64], out[64:128])
        ee = jnp.where(low, out[128:192], out[192:256])
        dd = dd + pltpu.roll(dd, 64, 1)
        ee = ee + pltpu.roll(ee, 64, 1)
        ee = pltpu.roll(ee, 32, 1)
        dd = dd + jnp.where(part == 0, -ee, ee)
        send4[4 * t:4 * t + 4] = jnp.where(low, dd[0:32], dd[32:64]).reshape(4, 8, 128)
        wait4.append(over_columns(3, t, send4, recv4))

    def columns_back(g):
        x4 = jnp.concatenate(unpack(recv4[4 * g:4 * g + 4].reshape(32, 128)), axis=0)
        y4 = pltpu.roll(x4, 32, 1)
        tiles = []
        for d in range(2):
            halves = []
            for half in range(2):
                a = []
                for k in range(4):
                    src = x4 if (k + d) % 2 == 0 else y4
                    a.append(src[32 * half + 8 * k:32 * half + 8 * k + 8])
                halves.append(
                    jnp.where(low, jnp.where(part == 0, a[0], a[1]), jnp.where(part == 0, a[2], a[3]))
                )
            tiles.append(jnp.concatenate(halves, axis=0))
        sre, sim = tiles
        for i in range(NI):
            wc = at[0, i:i + 1, span(128 * g, 128)]
            ws = at[1, i:i + 1, span(128 * g, 128)]
            put_left(ud, span(SLAB * i, SLAB), 0, sre * wc - sim * ws)
            put_left(ud, span(SLAB * i, SLAB), 128, sim * wc + sre * ws)
        return dot3(ud[...], bt[g])

    wait4[NEAR].wait_recv()
    near = columns_back(NEAR)
    for i in range(NI):
        rs = span(SLAB * i, SLAB)
        for d in range(2):
            new[d, :, LJ * i:LJ * (i + 1)] = (
                sky[d, :, LJ * i:LJ * (i + 1)] + near[rs, span(256 * d, 256)]
            )
    wait4[FAR].wait_recv()
    zs[...] = columns_back(FAR)
    for i in range(NI):
        rs = span(SLAB * i, SLAB)
        ur = new[0, :, LJ * i:LJ * (i + 1)] + zs[rs, 0:256]
        ui = new[1, :, LJ * i:LJ * (i + 1)] + zs[rs, 256:512]
        mag = jnp.sqrt(ur * ur + ui * ui)
        ratio = jnp.maximum(mag - SHRINK, 0.0) / jnp.maximum(mag, SHRINK)
        for d, x in enumerate((ur * ratio, ui * ratio)):
            new[d, :, LJ * i:LJ * (i + 1)] = x
            put_left(uu, rs, 256 * d, x)

    wait5 = []
    columns_forward(send5, lambda g: wait5.append(over_columns(4, g, send5, recv5)))
    wait6 = rows_forward(wait5, recv5, 5, send6, recv6)
    wait6[NEAR].wait_recv()
    for h, x in enumerate(model_half(NEAR, recv6[8:16], wz, tf, pt, zs, tt)):
        gs[span(256 * h, 256), :] = x
    wait6[FAR].wait_recv()
    parts[...] = recv6[0:8]
    for group in (wait1, wait2, wait3, wait4, wait5, wait6):
        for wait in group:
            wait.wait_send()


def local(sky_image, observed, weights, facet_offsets, subgrid_rows, subgrid_columns):
    vmem = pl.BlockSpec(memory_space=pltpu.VMEM)
    hbm = pl.BlockSpec(memory_space=pltpu.HBM)
    small = pltpu.VMEM((NC, 8, 128), F32)
    large = pltpu.VMEM((NF, SLAB, 128), F32)

    def left(rows, columns, *lead):
        return pltpu.VMEM((*lead, rows, 2 * columns), BF16)

    def right_of(rows, columns, *lead):
        return pltpu.VMEM((*lead, 3 * rows, columns), BF16)

    operands = [
        pltpu.with_memory_space_constraint(x, pltpu.HBM)
        for x in (facet_offsets.T, subgrid_rows, subgrid_columns, sky_image, observed, weights)
    ]
    halfway = pltpu.VMEM((512, 512), F32)
    parts, gs, wz, tf, pt, new = pl.pallas_call(
        kernel,
        out_shape=(
            pltpu.VMEM((8, SLAB, 128), F32),
            pltpu.VMEM((512, 512), F32),
            pltpu.VMEM((256, 512), BF16),
            pltpu.VMEM((2, NF, G), F32),
            left(512, 128, 2),
            pltpu.VMEM((2, SLAB, FN), F32),
        ),
        in_specs=[hbm] * 6,
        out_specs=(vmem,) * 6,
        scratch_shapes=[
            pltpu.SMEM((2, NF), jnp.int32),
            pltpu.SMEM((NF,), jnp.int32),
            pltpu.SMEM((NC,), jnp.int32),
            pltpu.VMEM((2, SLAB, FN), F32),
            pltpu.VMEM((2, G, G), F32),
            pltpu.VMEM((G, G), jnp.int32),
            right_of(512, 512),
            right_of(256, 512, 2),
            pltpu.VMEM((2, NI, LJ), F32),
            left(512, 128, 2),
            left(512, 128, 2),
            right_of(512, 128),
            left(512, 256),
            halfway,
            right_of(128, 512, 2),
            right_of(256, 512, 2),
            left(512, 512),
            left(512, 256),
            small, small, large, large, large, large, small, small, small, small, large, large,
            pltpu.SemaphoreType.DMA((6, 2)),
            pltpu.SemaphoreType.DMA((6, 2)),
            pltpu.SemaphoreType.DMA((6,)),
        ],
        compiler_params=pltpu.CompilerParams(
            collective_id=0, has_side_effects=True, vmem_limit_bytes=40 * 1024 * 1024
        ),
        name="imaging",
    )(*operands)
    return pl.pallas_call(
        finish_kernel,
        out_shape=(
            jax.ShapeDtypeStruct((2, SLAB, FN), F32),
            jax.ShapeDtypeStruct((2, G, G), F32),
        ),
        in_specs=[vmem] * 6,
        out_specs=(hbm, hbm),
        scratch_shapes=[
            pltpu.VMEM((2, G, G), F32),
            halfway,
            right_of(128, 512, 2),
            pltpu.SemaphoreType.DMA((5,)),
        ],
        compiler_params=pltpu.CompilerParams(vmem_limit_bytes=32 * 1024 * 1024),
        name="finish",
    )(parts, gs, wz, tf, pt, new)


def solution(mesh):
    return jax.shard_map(
        local,
        mesh=mesh,
        in_specs=(
            P(None, ("facet", "col"), None),
            P(None, "facet", "col"),
            P("facet", "col"),
            P(),
            P(),
            P(),
        ),
        out_specs=(P(None, ("facet", "col"), None), P(None, "facet", "col")),
        check_vma=False,
    )
```
